32 devices in a mesh: gx: 4 (over y, core), gy: 8 (over z, x).
Axes of the slice: x: 2, y: 2, z: 4, core: 2. Of those that a mesh axis runs over, the one named last changes fastest.
Arguments:
- tokens: bfloat16 [256, 4096], P('gy', 'gx'), may hold values from -140 to 140
- cotangent: bfloat16 [256, 4096], P('gy', 'gx'), may hold values from -6 to 6
- gate_weight: bfloat16 [4096, 14336], P('gx', 'gy'), may hold values from -5 to 5
- up_weight: bfloat16 [4096, 14336], P('gx', 'gy'), may hold values from -5 to 5
- down_weight: bfloat16 [14336, 4096], P('gy', 'gx'), may hold values from -5 to 5
Outputs:
- output: bfloat16 [256, 4096], P('gy', 'gx')
- input_grad: bfloat16 [256, 4096], P('gy', 'gx')
- gate_grad: bfloat16 [4096, 14336], P('gx', 'gy')
- up_grad: bfloat16 [4096, 14336], P('gx', 'gy')
- down_grad: bfloat16 [14336, 4096], P('gy', 'gx')
The draws below stay inside these ranges and needn't reach their ends.
All inputs are finite; a program needn't handle non-finite values.
Results may differ from the reference program's by a relative error of at most 0.005.
The reference program's roundings to bfloat16 on the way count: a program that leaves them out, or rounds other values in their place, can miss the bound.
Values may be sent and summed in bfloat16 or wider, within the bound.
A program may use at most 128 MiB of HBM per device.

```python
import jax
import jax.numpy as jnp
from jax import lax

D = 4096
FF = 14336
ROT_BLOCK = 128
HID_BLOCK = 64
TOKENS = 256


def rising_weight(key, row_total, col_total, fan_in):
    key_base, key_cols = jax.random.split(key)
    base = jnp.clip(jax.random.normal(key_base, (row_total, col_total), jnp.float32), -4.0, 4.0)
    row_frac = jnp.arange(row_total, dtype=jnp.float32)[:, None] / max(row_total - 1, 1)
    col_frac = jnp.arange(col_total, dtype=jnp.float32)[None, :] / max(col_total - 1, 1)
    col_rough = jnp.exp(jax.random.uniform(key_cols, (1, col_total), jnp.float32, 0.0, jnp.log(3.0)))
    rise = jnp.exp(jnp.log(3.0) * (row_frac + col_frac)) * col_rough
    return base * rise / (3.0 * fan_in ** 0.5)


def draw_tokens(key, part):
    key_base, key_rows, key_cols = jax.random.split(jax.random.fold_in(key, 11), 3)
    base = jnp.clip(jax.random.normal(key_base, (TOKENS, D), jnp.float32), -4.0, 4.0)
    row_rough = jnp.exp(jax.random.uniform(key_rows, (TOKENS, 1), jnp.float32, 0.0, jnp.log(3.3)))
    col_rough = jnp.exp(jax.random.uniform(key_cols, (1, D), jnp.float32, 0.0, jnp.log(3.0)))
    row_frac = jnp.arange(TOKENS, dtype=jnp.float32)[:, None] / max(TOKENS - 1, 1)
    col_frac = jnp.arange(D, dtype=jnp.float32)[None, :] / max(D - 1, 1)
    rise = jnp.exp(jnp.log(3.0) * (row_frac + col_frac))
    return (base * rise * row_rough * col_rough / 8.0).astype(jnp.bfloat16)


def draw_gate_weight(key, part):
    return rising_weight(jax.random.fold_in(key, 21), D, FF, D).astype(jnp.bfloat16)


def draw_up_weight(key, part):
    return rising_weight(jax.random.fold_in(key, 31), D, FF, D).astype(jnp.bfloat16)


def draw_down_weight(key, part):
    return rising_weight(jax.random.fold_in(key, 41), FF, D, FF).astype(jnp.bfloat16)


def block_levels(rng, extent, cuts, least, largest):
    loudness = 1.0
    for dim, parts in cuts:
        draws = jax.random.uniform(jax.random.fold_in(jax.random.fold_in(rng, 6), dim), (parts,), jnp.float32, least / len(cuts), largest / len(cuts))
        loudness = loudness * jnp.repeat(jnp.exp(draws), extent[dim] // parts).reshape((-1,) + (1,) * (len(extent) - 1 - dim))
    return loudness


def gaussian(own_key, shape, spread, most, cuts=(), kind=jnp.bfloat16):
    factor_of = block_levels(own_key, shape, cuts, -0.22, 0.18) if cuts else 1.0
    array = jax.random.normal(own_key, shape, jnp.float32) * spread * factor_of
    return jnp.minimum(jnp.maximum(array, -most), most).astype(kind)


def setup_inputs(seed: int = 0) -> dict:
    keys = jax.random.split(jax.random.key(seed), 6)
    return {
        "tokens": draw_tokens(jax.random.fold_in(keys[5], 71), 0),
        "cotangent": gaussian(keys[1], (TOKENS, D), 1.0, 6.0, ((0, 8), (1, 4))),
        "gate_weight": draw_gate_weight(jax.random.fold_in(keys[5], 71), 0),
        "up_weight": draw_up_weight(jax.random.fold_in(keys[5], 71), 0),
        "down_weight": draw_down_weight(jax.random.fold_in(keys[5], 71), 0),
    }


fp_top = 448.0
tiny = 1e-6


def hadamard_table(block_size):
    row_ids = jnp.arange(block_size, dtype=jnp.int32)[:, None]
    col_ids = jnp.arange(block_size, dtype=jnp.int32)[None, :]
    shared = row_ids & col_ids
    parity = jnp.zeros((block_size, block_size), jnp.int32)
    for bit_pos in range(max(block_size.bit_length() - 1, 1)):
        parity = parity + ((shared >> bit_pos) & 1)
    return (1 - 2 * (parity % 2)).astype(jnp.float32)


def rotate_cols(matrix, block_size):
    row_total, col_total = matrix.shape
    table = hadamard_table(block_size)
    blocks = matrix.astype(jnp.float32).reshape(row_total, col_total // block_size, block_size)
    turned = jnp.einsum("rbk,kl->rbl", blocks, table, precision=lax.Precision.HIGHEST)
    return turned.reshape(row_total, col_total) * (block_size ** -0.5)


def rotate_rows(matrix, block_size):
    row_total, col_total = matrix.shape
    table = hadamard_table(block_size)
    blocks = matrix.astype(jnp.float32).reshape(row_total // block_size, block_size, col_total)
    turned = jnp.einsum("kl,bkc->blc", table, blocks, precision=lax.Precision.HIGHEST)
    return turned.reshape(row_total, col_total) * (block_size ** -0.5)


def soft_cast(values, top):
    return (fp_top * jnp.tanh(values / (top + tiny))).astype(jnp.bfloat16)


def peak(values):
    return jnp.max(jnp.abs(values))


def reference(tokens, cotangent, gate_weight, up_weight, down_weight):
    token_rot = rotate_cols(tokens, ROT_BLOCK)
    gate_rot = rotate_rows(gate_weight, ROT_BLOCK)
    up_rot = rotate_rows(up_weight, ROT_BLOCK)
    down_rot = rotate_rows(down_weight, HID_BLOCK)
    token_peak = peak(token_rot)
    gate_peak = peak(gate_rot)
    up_peak = peak(up_rot)
    down_peak = peak(down_rot)
    token_cast = soft_cast(token_rot, token_peak)
    gate_cast = soft_cast(gate_rot, gate_peak)
    up_cast = soft_cast(up_rot, up_peak)
    down_cast = soft_cast(down_rot, down_peak)
    gate_pre = jnp.dot(token_cast, gate_cast, preferred_element_type=jnp.float32) * (token_peak * gate_peak / (fp_top * fp_top))
    up_pre = jnp.dot(token_cast, up_cast, preferred_element_type=jnp.float32) * (token_peak * up_peak / (fp_top * fp_top))
    hidden = (jax.nn.silu(gate_pre) * up_pre).astype(jnp.bfloat16)
    hidden_rot = rotate_cols(hidden, HID_BLOCK)
    hidden_peak = peak(hidden_rot)
    hidden_cast = soft_cast(hidden_rot, hidden_peak)
    output = (jnp.dot(hidden_cast, down_cast, preferred_element_type=jnp.float32) * (hidden_peak * down_peak / (fp_top * fp_top))).astype(jnp.bfloat16)
    down_grad = rotate_rows(jnp.dot(hidden_cast.T, cotangent, preferred_element_type=jnp.float32) * (hidden_peak / fp_top), HID_BLOCK).astype(jnp.bfloat16)
    hidden_grad = rotate_cols(jnp.dot(cotangent, down_cast.T, preferred_element_type=jnp.float32) * (down_peak / fp_top), HID_BLOCK)
    sigmoid_gate = jax.nn.sigmoid(gate_pre)
    gate_act = (hidden_grad * up_pre * sigmoid_gate * (1.0 + gate_pre * (1.0 - sigmoid_gate))).astype(jnp.bfloat16)
    up_act = (hidden_grad * gate_pre * sigmoid_gate).astype(jnp.bfloat16)
    gate_grad = rotate_rows(jnp.dot(token_cast.T, gate_act, preferred_element_type=jnp.float32) * (token_peak / fp_top), ROT_BLOCK).astype(jnp.bfloat16)
    up_grad = rotate_rows(jnp.dot(token_cast.T, up_act, preferred_element_type=jnp.float32) * (token_peak / fp_top), ROT_BLOCK).astype(jnp.bfloat16)
    input_sum = jnp.dot(gate_act, gate_cast.T, preferred_element_type=jnp.float32) * (gate_peak / fp_top) + jnp.dot(up_act, up_cast.T, preferred_element_type=jnp.float32) * (up_peak / fp_top)
    input_grad = rotate_cols(input_sum, ROT_BLOCK).astype(jnp.bfloat16)
    return (output, input_grad, gate_grad, up_grad, down_grad)
```

```python
import functools

import jax
import jax.numpy as jnp
from jax import lax
from jax.experimental import pallas as pl
from jax.experimental.pallas import tpu as pltpu
from jax.sharding import PartitionSpec as P

ROT_BLOCK = 128
HID_BLOCK = 64
CORES = 2

fp_top = 448.0
tiny = 1e-06

MESH = pl.DeviceIdType.MESH
VMEM = pl.BlockSpec(memory_space=pltpu.VMEM)
ANY = pl.BlockSpec(memory_space=pl.ANY)
DMA = pltpu.SemaphoreType.DMA
F32 = jnp.float32
BF16 = jnp.bfloat16


def rot_table(size, block):
    shift = block.bit_length() - 1
    row = lax.broadcasted_iota(jnp.int32, (size, size), 0)
    col = lax.broadcasted_iota(jnp.int32, (size, size), 1)
    bits = row & col & (block - 1)
    bits = bits ^ (bits >> 4)
    bits = bits ^ (bits >> 2)
    bits = bits ^ (bits >> 1)
    sign = 1 - 2 * (bits & 1)
    return jnp.where((row >> shift) == (col >> shift), sign, 0).astype(F32).astype(BF16)


def dot(left, right):
    return jnp.dot(left, right, preferred_element_type=F32)


def dot_t(left, right):
    return lax.dot_general(
        left, right, (((1,), (1,)), ((), ())), preferred_element_type=F32
    )


def dot_wide(values, table):
    high = values.astype(BF16)
    rest = values - high.astype(F32)
    mid = rest.astype(BF16)
    low = (rest - mid.astype(F32)).astype(BF16)
    return dot(high, table) + (dot(mid, table) + dot(low, table))


def remote(src, dst, send, recv, target):
    return pltpu.make_async_remote_copy(
        src_ref=src, dst_ref=dst, send_sem=send, recv_sem=recv,
        device_id=target, device_id_type=MESH,
    )


def loop(low, high, body):
    def step(i, carry):
        body(i)
        return carry
    lax.fori_loop(low, high, step, 0)


def greet(n, me, axis):
    barrier = pltpu.get_barrier_semaphore()

    def hello(k):
        pl.semaphore_signal(
            barrier, inc=1, device_id={axis: lax.rem(me + k, n)}, device_id_type=MESH
        )

    loop(1, n, hello)


def exchange(n, me, axis, src, slots, send, recv):
    def copy(k, slot):
        return remote(
            src, slots.at[slot], send.at[k], recv.at[k], {axis: lax.rem(me + k, n)}
        )

    def start(k):
        copy(k, me).start()

    def finish(k):
        copy(k, lax.rem(me + n - k, n)).wait()

    return (lambda: loop(1, n, start)), (lambda: loop(1, n, finish))


def fold(values):
    rows, cols = values.shape
    return jnp.max(jnp.abs(values).reshape(rows // 8, 8, cols), axis=0)


def ds(i, size):
    return pl.ds(pl.multiple_of(i * size, size), size)


def peak_tile(values):
    rows = lax.broadcasted_iota(jnp.int32, (8, 128), 0)
    tile = jnp.full((8, 128), values[0], F32)
    for i, value in enumerate(values[1:], 1):
        tile = jnp.where(rows == i, value, tile)
    return tile


def tile_scalar(tile, i):
    return jnp.max(tile[i : i + 1, :])


def layer_kernel(dims, names, *refs):
    nx, ny, lanes, tl, wide, hid, piece, band = dims
    r = dict(zip(names, refs))
    total_t = tl * ny
    tc = total_t // nx
    nc = hid // piece
    nb = wide // band
    gx, gy = lax.axis_index("gx"), lax.axis_index("gy")
    tok_s, hid_s = ROT_BLOCK ** (-0.5), HID_BLOCK ** (-0.5)

    wg, wu, wd = r["wg"], r["wu"], r["wd"]
    gate_hbm, up_hbm, down_hbm = r["gate"], r["up"], r["down"]

    def load(i, c):
        cols = ds(c, piece)
        src, dst = [
            (gate_hbm.at[:, cols], wg.at[c]),
            (up_hbm.at[:, cols], wu.at[c]),
            (down_hbm.at[cols, :], wd.at[c]),
        ][i]
        return pltpu.make_async_copy(src, dst, r["load"].at[i, c])

    def start_loads(c):
        for i in range(3):
            load(i, c).start()

    loop(0, nc, start_loads)
    greet(nx, gx, "gx")
    greet(ny, gy, "gy")
    pl.semaphore_wait(pltpu.get_barrier_semaphore(), nx - 1 + ny - 1)

    g_outer = ny // lanes
    g_hi, g_lo = gy // lanes, lax.rem(gy, lanes)
    g_blocks, g_all = [r["tokens"], r["cot"]], [r["all_tok"], r["all_cot"]]

    def g_far(i, k, slot):
        j = lax.rem(g_hi + k, g_outer)
        return remote(
            g_blocks[i], g_all[i].at[slot], r["g_sf"].at[i, k], r["g_rf"].at[i, k],
            {"gy": lanes * j + g_lo},
        )

    def g_near(i, k, o, src, slot):
        return remote(
            src, g_all[i].at[slot], r["g_sn"].at[i, k, o], r["g_rn"].at[i, k, o],
            {"gy": lanes * g_hi + lax.rem(g_lo + o, lanes)},
        )

    for i in range(2):
        for k in range(1, g_outer):
            g_far(i, k, gy).start()
        for o in range(1, lanes):
            g_near(i, 0, o, g_blocks[i], gy).start()

    def g_forward(k):
        mine = lanes * lax.rem(g_hi + g_outer - k, g_outer) + g_lo
        for i in range(2):
            g_far(i, k, mine).wait()
            for o in range(1, lanes):
                g_near(i, k, o, g_all[i].at[mine], mine).start()

    def g_finish(i):
        for o in range(1, lanes):
            side = lax.rem(g_lo + lanes - o, lanes)
            g_near(i, 0, o, g_blocks[i], lanes * g_hi + side).wait()
            for k in range(1, g_outer):
                row = lanes * lax.rem(g_hi + g_outer - k, g_outer)
                g_near(i, k, o, g_all[i].at[row + g_lo], row + side).wait()

    r["tab_w"][...] = rot_table(band, ROT_BLOCK)
    r["tab_h"][...] = rot_table(piece, HID_BLOCK)
    for i in range(2):
        g_all[i][gy] = g_blocks[i][...]
    tok_top = jnp.zeros((8, band), F32)
    for b in range(nb):
        cols = slice(b * band, (b + 1) * band)
        tok_top = jnp.maximum(tok_top, fold(dot(r["tokens"][:, cols], r["tab_w"][...])))

    def peak_step(c, tops):
        gate_top, up_top, down_top = tops
        for i in range(3):
            load(i, c).wait()
        for b in range(nb):
            rows = slice(b * band, (b + 1) * band)
            gate_top = jnp.maximum(gate_top, fold(dot(r["tab_w"][...], wg[c, rows, :])))
            up_top = jnp.maximum(up_top, fold(dot(r["tab_w"][...], wu[c, rows, :])))
            down_top = jnp.maximum(down_top, fold(dot(r["tab_h"][...], wd[c, :, rows])))
        return gate_top, up_top, down_top

    tops = (
        jnp.zeros((8, piece), F32), jnp.zeros((8, piece), F32), jnp.zeros((8, band), F32)
    )
    tops = lax.fori_loop(0, nc, peak_step, tops)
    r["tile"][...] = peak_tile([
        jnp.max(tok_top) * tok_s, jnp.max(tops[0]) * tok_s,
        jnp.max(tops[1]) * tok_s, jnp.max(tops[2]) * hid_s,
    ])
    start_x, finish_x = exchange(nx, gx, "gx", r["tile"], r["slots_x"], r["p_sx"], r["p_rx"])
    start_y, finish_y = exchange(ny, gy, "gy", r["mid"], r["slots_y"], r["p_sy"], r["p_ry"])
    start_x()
    r["slots_x"][gx] = r["tile"][...]
    loop(1, g_outer, g_forward)
    finish_x()
    r["mid"][...] = jnp.max(r["slots_x"][...], axis=0)
    start_y()
    r["slots_y"][gy] = r["mid"][...]
    g_finish(0)
    finish_y()
    top = jnp.max(r["slots_y"][...], axis=0)
    inverse = 1.0 / (top + tiny)
    unit = top / fp_top
    pair = top[0:1, :] * top / (fp_top * fp_top)
    tok_inv = tile_scalar(inverse, 0) * tok_s
    gate_inv = tile_scalar(inverse, 1) * tok_s
    up_inv = tile_scalar(inverse, 2) * tok_s
    down_inv = tile_scalar(inverse, 3) * hid_s
    tok_unit, gate_unit, up_unit, down_unit = (tile_scalar(unit, i) for i in range(4))
    gate_scale, up_scale = tile_scalar(pair, 1), tile_scalar(pair, 2)

    def soft(values):
        return (fp_top * jnp.tanh(values)).astype(BF16)

    for b in range(nb):
        cols = slice(b * band, (b + 1) * band)
        raw = r["all_tok"][:, :, cols].reshape(total_t, band)
        r["tok"][:, cols] = soft(dot(raw, r["tab_w"][...]) * tok_inv)

    def cast_step(c):
        for b in range(nb):
            rows = slice(b * band, (b + 1) * band)
            wg[c, rows, :] = soft(dot(r["tab_w"][...], wg[c, rows, :]) * gate_inv)
            wu[c, rows, :] = soft(dot(r["tab_w"][...], wu[c, rows, :]) * up_inv)
            wd[c, :, rows] = soft(dot(r["tab_h"][...], wd[c, :, rows]) * down_inv)

    x_outer = nx // CORES
    x_hi, x_lo = gx // CORES, lax.rem(gx, CORES)
    x_order = list(range(1, x_outer)) + [0]
    part, first, second, third, act = (
        r["part"], r["first"], r["second"], r["third"], r["act"]
    )

    def s_near(c, k, o):
        j, to = lax.rem(x_hi + k, x_outer), lax.rem(x_lo + o, CORES)
        return remote(
            part.at[c, CORES * j + to], first.at[c, k, o - 1], r["s_s1"].at[c, k, o],
            r["s_r1"].at[c, k, o], {"gx": CORES * x_hi + to},
        )

    def s_far(c, k):
        j = lax.rem(x_hi + k, x_outer)
        return remote(
            second.at[c, k - 1], third.at[c, k - 1], r["s_s2"].at[c, k],
            r["s_r2"].at[c, k], {"gx": CORES * j + x_lo},
        )

    def a_far(c, k, slot):
        j = lax.rem(x_hi + k, x_outer)
        return remote(
            act.at[c, slot], act.at[c, slot], r["a_sf"].at[c, k], r["a_rf"].at[c, k],
            {"gx": CORES * j + x_lo},
        )

    def a_near(c, k, o, slot):
        return remote(
            act.at[c, slot], act.at[c, slot], r["a_sn"].at[c, k, o], r["a_rn"].at[c, k, o],
            {"gx": CORES * x_hi + lax.rem(x_lo + o, CORES)},
        )

    def matmul_step(c):
        for i in range(3):
            if i == 2:
                total = dot_t(r["all_cot"][...].reshape(total_t, wide), wd[c])
            else:
                total = dot(r["tok"][...], (wg, wu)[i][c])
            part[c, :, i] = total.reshape(nx, tc, piece)
        for k in x_order:
            for o in range(1, CORES):
                s_near(c, k, o).start()

    def near_sum(c, k, i):
        total = part[c, CORES * lax.rem(x_hi + k, x_outer) + x_lo, i]
        for o in range(1, CORES):
            total = total + first[c, k, o - 1, i]
        return total

    def pass_step(c):
        for k in x_order[:-1]:
            for o in range(1, CORES):
                s_near(c, k, o).wait()
            for i in range(3):
                second[c, k - 1, i] = near_sum(c, k, i).astype(BF16)
            s_far(c, k).start()

    def act_step(c):
        for o in range(1, CORES):
            s_near(c, 0, o).wait()
        for k in x_order[:-1]:
            s_far(c, k).wait()

        def full(i):
            total = near_sum(c, 0, i)
            for k in x_order[:-1]:
                total = total + third[c, k - 1, i].astype(F32)
            return total

        gate_pre = full(0) * gate_scale
        up_pre = full(1) * up_scale
        sig = jax.nn.sigmoid(gate_pre)
        hidden = (gate_pre * sig * up_pre).astype(BF16)
        act[c, gx, 0] = hidden
        grad = dot_wide(full(2) * down_unit, r["tab_h"][...]) * hid_s
        act[c, gx, 1] = (
            grad * up_pre * sig * (1.0 + gate_pre * (1.0 - sig))
        ).astype(BF16)
        act[c, gx, 2] = (grad * gate_pre * sig).astype(BF16)
        for k in range(1, x_outer):
            a_far(c, k, gx).start()
        for o in range(1, CORES):
            a_near(c, 0, o, gx).start()
        r["top_h"][...] = jnp.maximum(
            r["top_h"][...], fold(dot(hidden, r["tab_h"][...]))
        )

    def forward_step(c):
        for k in range(1, x_outer):
            mine = CORES * lax.rem(x_hi + x_outer - k, x_outer) + x_lo
            a_far(c, k, mine).wait()
            for o in range(1, CORES):
                a_near(c, k, o, mine).start()

    def arrive_step(c):
        for o in range(1, CORES):
            side = lax.rem(x_lo + CORES - o, CORES)
            for k in range(x_outer):
                row = CORES * lax.rem(x_hi + x_outer - k, x_outer)
                a_near(c, k, o, row + side).wait()

    r["top_h"][...] = jnp.zeros((8, piece), F32)
    cast_step(0)
    g_finish(1)

    def pipeline(i):
        @pl.when(i < nc)
        def _():
            matmul_step(i)

        @pl.when(i + 1 < nc)
        def _():
            cast_step(i + 1)

        @pl.when(i < nc)
        def _():
            pass_step(i)

        @pl.when((i >= 1) & (i < nc + 1))
        def _():
            act_step(i - 1)

        @pl.when(i >= 2)
        def _():
            forward_step(i - 2)

    loop(0, nc + 2, pipeline)

    r["tile2"][...] = peak_tile([jnp.max(r["top_h"][...]) * hid_s])
    start_y2, finish_y2 = exchange(
        ny, gy, "gy", r["tile2"], r["slots_y2"], r["q_sy"], r["q_ry"]
    )
    start_x2, finish_x2 = exchange(
        nx, gx, "gx", r["mid2"], r["slots_x2"], r["q_sx"], r["q_rx"]
    )
    start_y2()
    r["slots_y2"][gy] = r["tile2"][...]
    loop(0, nc, arrive_step)

    y_outer = ny // lanes
    y_order = list(range(1, y_outer)) + [0]
    bufs = [r["out_part"], r["in_part"]]
    ones, twos, threes = r["y_one"], r["y_two"], r["y_three"]

    def y_near(i, k, o):
        j, to = lax.rem(g_hi + k, y_outer), lax.rem(g_lo + o, lanes)
        return remote(
            bufs[i].at[lanes * j + to], ones.at[i, k, o - 1], r["y_s1"].at[i, k, o],
            r["y_r1"].at[i, k, o], {"gy": lanes * g_hi + to},
        )

    def y_far(i, k):
        j = lax.rem(g_hi + k, y_outer)
        return remote(
            twos.at[i, k - 1], threes.at[i, k - 1], r["y_s2"].at[i, k],
            r["y_r2"].at[i, k], {"gy": lanes * j + g_lo},
        )

    def y_send(i):
        for k in y_order:
            for o in range(1, lanes):
                y_near(i, k, o).start()

    def y_sum(i, k):
        total = bufs[i][lanes * lax.rem(g_hi + k, y_outer) + g_lo].astype(F32)
        for o in range(1, lanes):
            total = total + ones[i, k, o - 1].astype(F32)
        return total

    def y_pass(i, k):
        for o in range(1, lanes):
            y_near(i, k, o).wait()
        twos[i, k - 1] = y_sum(i, k).astype(BF16)
        y_far(i, k).start()

    def y_close(i):
        for o in range(1, lanes):
            y_near(i, 0, o).wait()
        total = y_sum(i, 0)
        for k in y_order[:-1]:
            y_far(i, k).wait()
            total = total + threes[i, k - 1].astype(F32)
        return total

    def rows_of(c, i):
        return act[c, :, i].reshape(total_t, piece)

    def in_step(b):
        rows = ds(b, band)
        gate_sum = jnp.zeros((total_t, band), F32)
        up_sum = jnp.zeros((total_t, band), F32)
        for c in range(nc):
            gate_sum = gate_sum + dot_t(rows_of(c, 1), wg[c, rows, :])
            up_sum = up_sum + dot_t(rows_of(c, 2), wu[c, rows, :])
        total = gate_sum * gate_unit + up_sum * up_unit
        r["in_part"][:, :, rows] = total.astype(BF16).reshape(ny, tl, band)

    loop(0, nb, in_step)
    y_send(1)
    finish_y2()
    r["mid2"][...] = jnp.max(r["slots_y2"][...], axis=0)
    start_x2()
    r["slots_x2"][gx] = r["mid2"][...]

    for b in range(nb):
        cols = slice(b * band, (b + 1) * band)
        turned = dot(r["tok"][:, cols], r["tab_w"][...]) * tok_s
        r["tok_t"][cols, :] = turned.T.astype(BF16)

    gate_out, up_out, down_out = r["gate_grad"], r["up_grad"], r["down_grad"]

    def store(i, c):
        cols = ds(c, piece)
        src, dst = [
            (wg.at[c], gate_out.at[:, cols]),
            (wu.at[c], up_out.at[:, cols]),
            (wd.at[c], down_out.at[cols, :]),
        ][i]
        return pltpu.make_async_copy(src, dst, r["save"].at[i, c])

    def weight_grads(c):
        for b in range(nb):
            rows = slice(b * band, (b + 1) * band)
            wg[c, rows, :] = (
                dot(r["tok_t"][rows, :], rows_of(c, 1)) * tok_unit
            ).astype(BF16)
            wu[c, rows, :] = (
                dot(r["tok_t"][rows, :], rows_of(c, 2)) * tok_unit
            ).astype(BF16)
        store(0, c).start()
        store(1, c).start()

    finish_x2()
    top2 = jnp.max(r["slots_x2"][...], axis=0)
    hidden_inv = tile_scalar(1.0 / (top2 + tiny), 0) * hid_s
    hidden_unit = tile_scalar(top2 / fp_top, 0)
    out_scale = tile_scalar(top2[0:1, :] * top[3:4, :] / (fp_top * fp_top), 0)

    def hidden_step(c):
        r["hid"][c] = soft(dot(rows_of(c, 0), r["tab_h"][...]) * hidden_inv)

    loop(0, nc, hidden_step)

    def out_step(b):
        cols = ds(b, band)
        total = jnp.zeros((total_t, band), F32)
        for c in range(nc):
            total = total + dot(r["hid"][c], wd[c, :, cols])
        r["out_part"][:, :, cols] = total.astype(BF16).reshape(ny, tl, band)

    loop(0, nb, out_step)
    y_send(0)

    def down_grads(c):
        turned = (dot(r["hid"][c], r["tab_h"][...]) * hid_s).T.astype(BF16)
        cot = r["all_cot"][...].reshape(total_t, wide)
        wd[c] = (dot(turned, cot) * hidden_unit).astype(BF16)
        store(2, c).start()

    cuts = [nc * k // y_outer for k in range(y_outer + 1)]
    for n, k in enumerate(y_order):
        loop(cuts[n], cuts[n + 1], weight_grads)
        if k:
            y_pass(1, k)
    for n, k in enumerate(y_order):
        loop(cuts[n], cuts[n + 1], down_grads)
        if k:
            y_pass(0, k)

    total = y_close(1)
    for b in range(nb):
        cols = slice(b * band, (b + 1) * band)
        r["input_grad"][:, cols] = (
            dot_wide(total[:, cols], r["tab_w"][...]) * tok_s
        ).astype(BF16)
    r["output"][...] = (y_close(0) * out_scale).astype(BF16)

    def drain(c):
        for i in range(3):
            store(i, c).wait()

    loop(0, nc, drain)


def shards(nx, ny, tokens, cotangent, gate_weight, up_weight, down_weight):
    lanes = 1 << max((ny.bit_length() - 2) // 2, 0)
    tl, wide = tokens.shape
    hid = gate_weight.shape[1]
    piece = 256 if hid % 256 == 0 else hid
    band = 256 if wide % 256 == 0 else wide
    nc = hid // piece
    total_t = tl * ny
    tc = total_t // nx
    x_outer, y_outer = nx // CORES, ny // lanes
    dims = (nx, ny, lanes, tl, wide, hid, piece, band)
    ins = ["tokens", "cot", "gate", "up", "down"]
    outs = ["output", "input_grad", "gate_grad", "up_grad", "down_grad"]
    tile = pltpu.VMEM((8, 128), F32)
    scratch = {
        "wg": pltpu.VMEM((nc, wide, piece), BF16),
        "wu": pltpu.VMEM((nc, wide, piece), BF16),
        "wd": pltpu.VMEM((nc, piece, wide), BF16),
        "load": DMA((3, nc)),
        "save": DMA((3, nc)),
        "all_tok": pltpu.VMEM((ny, tl, wide), BF16),
        "all_cot": pltpu.VMEM((ny, tl, wide), BF16),
        "g_sf": DMA((2, y_outer)), "g_rf": DMA((2, y_outer)),
        "g_sn": DMA((2, y_outer, lanes)), "g_rn": DMA((2, y_outer, lanes)),
        "tab_w": pltpu.VMEM((band, band), BF16),
        "tab_h": pltpu.VMEM((piece, piece), BF16),
        "tile": tile, "mid": tile, "tile2": tile, "mid2": tile,
        "slots_x": pltpu.VMEM((nx, 8, 128), F32),
        "slots_y": pltpu.VMEM((ny, 8, 128), F32),
        "slots_x2": pltpu.VMEM((nx, 8, 128), F32),
        "slots_y2": pltpu.VMEM((ny, 8, 128), F32),
        "p_sx": DMA((nx,)), "p_rx": DMA((nx,)), "p_sy": DMA((ny,)), "p_ry": DMA((ny,)),
        "q_sx": DMA((nx,)), "q_rx": DMA((nx,)), "q_sy": DMA((ny,)), "q_ry": DMA((ny,)),
        "tok": pltpu.VMEM((total_t, wide), BF16),
        "tok_t": pltpu.VMEM((wide, total_t), BF16),
        "part": pltpu.VMEM((nc, nx, 3, tc, piece), F32),
        "first": pltpu.VMEM((nc, x_outer, CORES - 1, 3, tc, piece), F32),
        "second": pltpu.VMEM((nc, x_outer - 1, 3, tc, piece), BF16),
        "third": pltpu.VMEM((nc, x_outer - 1, 3, tc, piece), BF16),
        "act": pltpu.VMEM((nc, nx, 3, tc, piece), BF16),
        "hid": pltpu.VMEM((nc, total_t, piece), BF16),
        "s_s1": DMA((nc, x_outer, CORES)), "s_r1": DMA((nc, x_outer, CORES)),
        "s_s2": DMA((nc, x_outer)), "s_r2": DMA((nc, x_outer)),
        "a_sf": DMA((nc, x_outer)), "a_rf": DMA((nc, x_outer)),
        "a_sn": DMA((nc, x_outer, CORES)), "a_rn": DMA((nc, x_outer, CORES)),
        "top_h": pltpu.VMEM((8, piece), F32),
        "out_part": pltpu.VMEM((ny, tl, wide), BF16),
        "in_part": pltpu.VMEM((ny, tl, wide), BF16),
        "y_one": pltpu.VMEM((2, y_outer, lanes - 1, tl, wide), BF16),
        "y_two": pltpu.VMEM((2, y_outer - 1, tl, wide), BF16),
        "y_three": pltpu.VMEM((2, y_outer - 1, tl, wide), BF16),
        "y_s1": DMA((2, y_outer, lanes)), "y_r1": DMA((2, y_outer, lanes)),
        "y_s2": DMA((2, y_outer)), "y_r2": DMA((2, y_outer)),
    }
    names = tuple(ins + outs + list(scratch))
    small = jax.ShapeDtypeStruct(tokens.shape, BF16)
    return pl.pallas_call(
        functools.partial(layer_kernel, dims, names),
        out_shape=[small, small] + [
            jax.ShapeDtypeStruct(w.shape, BF16)
            for w in (gate_weight, up_weight, down_weight)
        ],
        in_specs=[VMEM, VMEM, ANY, ANY, ANY],
        out_specs=[VMEM, VMEM, ANY, ANY, ANY],
        scratch_shapes=list(scratch.values()),
        compiler_params=pltpu.CompilerParams(
            collective_id=0, has_side_effects=True, vmem_limit_bytes=62 * 2 ** 20
        ),
    )(tokens, cotangent, gate_weight, up_weight, down_weight)


def solution(mesh):
    in_specs = (P("gy", "gx"), P("gy", "gx"), P("gx", "gy"), P("gx", "gy"), P("gy", "gx"))
    out_specs = (P("gy", "gx"), P("gy", "gx"), P("gx", "gy"), P("gx", "gy"), P("gy", "gx"))
    nx, ny = mesh.shape["gx"], mesh.shape["gy"]
    return jax.shard_map(
        functools.partial(shards, nx, ny),
        mesh=mesh, in_specs=in_specs, out_specs=out_specs, check_vma=False,
    )
```

```python
import functools

import jax
import jax.numpy as jnp
from jax import lax
from jax.experimental import pallas as pl
from jax.experimental.pallas import tpu as pltpu
from jax.sharding import PartitionSpec as P

ROT_BLOCK = 128
HID_BLOCK = 64
CORES = 2
VMEM_MIB = 50
STORE_MIB = 12
LAG = 2

fp_top = 448.0
tiny = 1e-06

MESH = pl.DeviceIdType.MESH
VMEM = pl.BlockSpec(memory_space=pltpu.VMEM)
HBM = pl.BlockSpec(memory_space=pltpu.HBM)
DMA = pltpu.SemaphoreType.DMA
F32 = jnp.float32
BF16 = jnp.bfloat16


def rot_table(size, block):
    shift = block.bit_length() - 1
    row = lax.broadcasted_iota(jnp.int32, (size, size), 0)
    col = lax.broadcasted_iota(jnp.int32, (size, size), 1)
    bits = row & col & (block - 1)
    bits = bits ^ (bits >> 4)
    bits = bits ^ (bits >> 2)
    bits = bits ^ (bits >> 1)
    sign = 1 - 2 * (bits & 1)
    return jnp.where((row >> shift) == (col >> shift), sign, 0).astype(F32).astype(BF16)


def dot(left, right):
    return jnp.dot(left, right, preferred_element_type=F32)


def dot_t(left, right):
    return lax.dot_general(
        left, right, (((1,), (1,)), ((), ())), preferred_element_type=F32
    )


def dot_wide(values, table):
    high = values.astype(BF16)
    rest = values - high.astype(F32)
    mid = rest.astype(BF16)
    low = (rest - mid.astype(F32)).astype(BF16)
    return dot(high, table) + (dot(mid, table) + dot(low, table))


def remote(src, dst, send, recv, target):
    return pltpu.make_async_remote_copy(
        src_ref=src, dst_ref=dst, send_sem=send, recv_sem=recv,
        device_id=target, device_id_type=MESH,
    )


def loop(low, high, body):
    def step(i, carry):
        body(i)
        return carry
    lax.fori_loop(low, high, step, 0)


def greet(n, me, axis):
    barrier = pltpu.get_barrier_semaphore()

    def hello(k):
        pl.semaphore_signal(
            barrier, inc=1, device_id={axis: lax.rem(me + k, n)}, device_id_type=MESH
        )

    loop(1, n, hello)


def take(ref, sem):
    pltpu.make_async_copy(ref, ref, sem).wait()


def exchange(n, me, axis, src, slots, sems):
    def start(k):
        target = {axis: lax.rem(me + k, n)}
        remote(src, slots.at[k], sems.at[0], sems.at[1], target).start()

    def finish():
        rest = slots.at[pl.ds(1, n - 1)]
        take(rest, sems.at[0])
        take(rest, sems.at[1])

    return (lambda: loop(1, n, start)), finish


def fold(values):
    rows, cols = values.shape
    return jnp.max(jnp.abs(values).reshape(rows // 8, 8, cols), axis=0)


def ds(i, size):
    return pl.ds(pl.multiple_of(i * size, size), size)


def peak_tile(values):
    rows = lax.broadcasted_iota(jnp.int32, (8, 128), 0)
    tile = jnp.full((8, 128), values[0], F32)
    for i, value in enumerate(values[1:], 1):
        tile = jnp.where(rows == i, value, tile)
    return tile


def tile_scalar(tile, i):
    return jnp.max(tile[i : i + 1, :])


def layer_kernel(dims, names, *refs):
    nx, ny, lanes, tl, wide, hid, piece, band = dims
    r = dict(zip(names, refs))
    total_t = tl * ny
    tc = total_t // nx
    nc = hid // piece
    nb = wide // band
    gx, gy = lax.axis_index("gx"), lax.axis_index("gy")
    tok_s, hid_s = ROT_BLOCK ** (-0.5), HID_BLOCK ** (-0.5)
    wg, wu, wd = r["wg"], r["wu"], r["wd"]
    all_tok, all_cot = r["all_tok"], r["all_cot"]

    def own_load(i):
        src, dst = ((r["tokens"], all_tok), (r["cot"], all_cot))[i]
        return pltpu.make_async_copy(src, dst.at[gy], r["own"].at[i])

    own_load(0).start()
    own_load(1).start()
    greet(nx, gx, "gx")
    greet(ny, gy, "gy")

    def load(i, c):
        cols = ds(c, piece)
        src, dst = [
            (r["gate"].at[:, cols], wg.at[c]),
            (r["up"].at[:, cols], wu.at[c]),
            (r["down"].at[cols, :], wd.at[c]),
        ][i]
        return pltpu.make_async_copy(src, dst, r["load"].at[i, c])

    def start_loads(c):
        for i in range(3):
            load(i, c).start()

    loop(0, nc, start_loads)
    r["tab_w"][...] = rot_table(band, ROT_BLOCK)
    r["tab_h"][...] = rot_table(piece, HID_BLOCK)
    own_load(0).wait()
    own_load(1).wait()
    pl.semaphore_wait(pltpu.get_barrier_semaphore(), nx - 1 + ny - 1)

    y_outer = ny // lanes
    y_hi, y_lo = gy // lanes, lax.rem(gy, lanes)
    g_all = [all_tok, all_cot]

    def g_far(i, k, slot):
        j = lax.rem(y_hi + k, y_outer)
        return remote(
            g_all[i].at[slot], g_all[i].at[slot], r["g_sf"].at[i], r["g_rf"].at[i, k - 1],
            {"gy": lanes * j + y_lo},
        )

    def g_near(i, o, slot):
        return remote(
            g_all[i].at[slot], g_all[i].at[slot], r["g_sn"].at[i],
            r["g_rn"].at[i], {"gy": lanes * y_hi + lax.rem(y_lo + o, lanes)},
        )

    def g_start(i):
        for k in range(1, y_outer):
            g_far(i, k, gy).start()
        for o in range(1, lanes):
            g_near(i, o, gy).start()

    def g_forward(i, k):
        mine = lanes * lax.rem(y_hi + y_outer - k, y_outer) + y_lo
        g_far(i, k, mine).wait_recv()
        for o in range(1, lanes):
            g_near(i, o, mine).start()

    def g_finish(i):
        take(g_all[i].at[pl.ds(0, y_outer * (lanes - 1))], r["g_rn"].at[i])

    def g_drain(i):
        take(g_all[i].at[pl.ds(0, y_outer - 1)], r["g_sf"].at[i])
        take(g_all[i].at[pl.ds(0, y_outer * (lanes - 1))], r["g_sn"].at[i])

    g_start(0)

    tok_top = jnp.zeros((8, band), F32)
    for b in range(nb):
        cols = slice(b * band, (b + 1) * band)
        tok_top = jnp.maximum(tok_top, fold(dot(all_tok[gy, :, cols], r["tab_w"][...])))

    def peak_step(c, tops):
        gate_top, up_top, down_top = tops
        for i in range(3):
            load(i, c).wait()
        for b in range(nb):
            rows = slice(b * band, (b + 1) * band)
            gate_top = jnp.maximum(gate_top, fold(dot(r["tab_w"][...], wg[c, rows, :])))
            up_top = jnp.maximum(up_top, fold(dot(r["tab_w"][...], wu[c, rows, :])))
            down_top = jnp.maximum(down_top, fold(dot(r["tab_h"][...], wd[c, :, rows])))
        return gate_top, up_top, down_top

    tops = (
        jnp.zeros((8, piece), F32), jnp.zeros((8, piece), F32), jnp.zeros((8, band), F32)
    )
    tops = lax.fori_loop(0, nc, peak_step, tops)
    r["tile"][...] = peak_tile([
        jnp.max(tok_top) * tok_s, jnp.max(tops[0]) * tok_s,
        jnp.max(tops[1]) * tok_s, jnp.max(tops[2]) * hid_s,
    ])
    start_x, finish_x = exchange(nx, gx, "gx", r["tile"], r["slots_x"], r["p_x"])
    start_y, finish_y = exchange(ny, gy, "gy", r["mid"], r["slots_y"], r["p_y"])
    start_x()
    r["slots_x"][0] = r["tile"][...]
    for k in range(1, y_outer - 1):
        g_forward(0, k)
    finish_x()
    r["mid"][...] = jnp.max(r["slots_x"][...], axis=0)
    start_y()
    r["slots_y"][0] = r["mid"][...]
    g_forward(0, y_outer - 1)
    g_start(1)
    g_finish(0)
    finish_y()
    top = jnp.max(r["slots_y"][...], axis=0)
    inverse = 1.0 / (top + tiny)
    unit = top / fp_top
    pair = top[0:1, :] * top / (fp_top * fp_top)
    tok_inv = tile_scalar(inverse, 0) * tok_s
    gate_inv = tile_scalar(inverse, 1) * tok_s
    up_inv = tile_scalar(inverse, 2) * tok_s
    down_inv = tile_scalar(inverse, 3) * hid_s
    tok_unit, gate_unit, up_unit, down_unit = (tile_scalar(unit, i) for i in range(4))
    gate_scale, up_scale = tile_scalar(pair, 1), tile_scalar(pair, 2)

    def soft(values):
        return (fp_top * jnp.tanh(values)).astype(BF16)

    for b in range(nb):
        cols = slice(b * band, (b + 1) * band)
        raw = all_tok[:, :, cols].reshape(total_t, band)
        r["tok"][:, cols] = soft(dot(raw, r["tab_w"][...]) * tok_inv)

    def cast_gate_up(c):
        for b in range(nb):
            rows = slice(b * band, (b + 1) * band)
            wg[c, rows, :] = soft(dot(r["tab_w"][...], wg[c, rows, :]) * gate_inv)
            wu[c, rows, :] = soft(dot(r["tab_w"][...], wu[c, rows, :]) * up_inv)

    def cast_down(c):
        for b in range(nb):
            rows = slice(b * band, (b + 1) * band)
            wd[c, :, rows] = soft(dot(r["tab_h"][...], wd[c, :, rows]) * down_inv)

    x_outer = nx // CORES
    x_hi, x_lo = gx // CORES, lax.rem(gx, CORES)
    x_order = list(range(1, x_outer)) + [0]

    class Sums:
        def __init__(self, tag, count):
            self.count = count
            self.part, self.first = r[tag + "_part"], r[tag + "_first"]
            self.second, self.third = r[tag + "_second"], r[tag + "_third"]
            self.s1, self.r1 = r[tag + "_s"].at[0], r[tag + "_r1"]
            self.s2, self.r2 = r[tag + "_s"].at[1], r[tag + "_r2"]

        def near(self, c, k, o):
            j, to = lax.rem(x_hi + k, x_outer), lax.rem(x_lo + o, CORES)
            return remote(
                self.part.at[c, CORES * j + to], self.first.at[c, k, o - 1],
                self.s1, self.r1.at[c, k], {"gx": CORES * x_hi + to},
            )

        def far(self, c, k):
            j = lax.rem(x_hi + k, x_outer)
            return remote(
                self.second.at[c, k - 1], self.third.at[c, k - 1], self.s2,
                self.r2.at[c, k - 1], {"gx": CORES * j + x_lo},
            )

        def send(self, c):
            for k in x_order:
                for o in range(1, CORES):
                    self.near(c, k, o).start()

        def near_sum(self, c, k, i):
            total = self.part[c, CORES * lax.rem(x_hi + k, x_outer) + x_lo, i]
            for o in range(1, CORES):
                total = total + self.first[c, k, o - 1, i]
            return total

        def turn(self, c):
            for k in x_order[:-1]:
                take(self.first.at[c, k], self.r1.at[c, k])
                for i in range(self.count):
                    self.second[c, k - 1, i] = self.near_sum(c, k, i).astype(BF16)
                self.far(c, k).start()

        def close(self, c):
            take(self.first.at[c, 0], self.r1.at[c, 0])
            for k in x_order[:-1]:
                self.far(c, k).wait_recv()

        def drain(self):
            take(self.first, self.s1)
            take(self.third, self.s2)

        def full(self, c, i):
            total = self.near_sum(c, 0, i)
            for k in x_order[:-1]:
                total = total + self.third[c, k - 1, i].astype(F32)
            return total

    class Spread:
        def __init__(self, tag):
            self.act = r[tag]
            self.sf, self.rf = r[tag + "_s"].at[0], r[tag + "_rf"]
            self.sn, self.rn = r[tag + "_s"].at[1], r[tag + "_rn"]

        def far(self, c, k, slot):
            j = lax.rem(x_hi + k, x_outer)
            return remote(
                self.act.at[c, slot], self.act.at[c, slot], self.sf,
                self.rf.at[c, k - 1], {"gx": CORES * j + x_lo},
            )

        def near(self, c, o, slot):
            return remote(
                self.act.at[c, slot], self.act.at[c, slot], self.sn,
                self.rn.at[c], {"gx": CORES * x_hi + lax.rem(x_lo + o, CORES)},
            )

        def send(self, c):
            for k in range(1, x_outer):
                self.far(c, k, gx).start()
            for o in range(1, CORES):
                self.near(c, o, gx).start()

        def forward(self, c):
            for k in range(1, x_outer):
                mine = CORES * lax.rem(x_hi + x_outer - k, x_outer) + x_lo
                self.far(c, k, mine).wait_recv()
                for o in range(1, CORES):
                    self.near(c, o, mine).start()

        def arrive(self, c):
            take(self.act.at[c, pl.ds(0, x_outer * (CORES - 1))], self.rn.at[c])

        def drain(self):
            take(self.act.at[:, pl.ds(0, x_outer - 1)], self.sf)
            take(self.act.at[:, pl.ds(0, x_outer * (CORES - 1))], self.sn)

        def rows(self, c, i):
            return self.act[c, :, i].reshape(total_t, piece)

    pre, back = Sums("pre", 2), Sums("back", 1)
    hidden_out, grad_out = Spread("act_h"), Spread("act_g")

    def mm_pre(c):
        for i, weight in enumerate((wg, wu)):
            pre.part[c, :, i] = dot(r["tok"][...], weight[c]).reshape(nx, tc, piece)
        pre.send(c)

    def mm_back(c):
        cot = all_cot[...].reshape(total_t, wide)
        back.part[c, :, 0] = dot_t(cot, wd[c]).reshape(nx, tc, piece)
        back.send(c)

    def act_hidden(c):
        pre.close(c)
        gate_pre = pre.full(c, 0) * gate_scale
        up_pre = pre.full(c, 1) * up_scale
        sig = jax.nn.sigmoid(gate_pre)
        hidden = (gate_pre * sig * up_pre).astype(BF16)
        hidden_out.act[c, gx, 0] = hidden
        hidden_out.send(c)
        r["slope"][c, 0] = up_pre * sig * (1.0 + gate_pre * (1.0 - sig))
        r["slope"][c, 1] = gate_pre * sig
        r["top_h"][...] = jnp.maximum(
            r["top_h"][...], fold(dot(hidden, r["tab_h"][...]))
        )

    def act_grad(c):
        back.close(c)
        grad = dot_wide(back.full(c, 0) * down_unit, r["tab_h"][...]) * hid_s
        for i in range(2):
            grad_out.act[c, gx, i] = (grad * r["slope"][c, i]).astype(BF16)
        grad_out.send(c)

    r["top_h"][...] = jnp.zeros((8, piece), F32)

    def when(cond, body, *args):
        @pl.when(cond)
        def _():
            body(*args)

    lead = 3
    inside = max(0, min(y_outer - 1, nc - lead))

    def cot_ready():
        for k in range(inside + 1, y_outer):
            g_forward(1, k)
        g_finish(1)

    start_y2, finish_y2 = exchange(
        ny, gy, "gy", r["tile2"], r["slots_y2"], r["q_y"]
    )
    start_x2, finish_x2 = exchange(
        nx, gx, "gx", r["mid2"], r["slots_x2"], r["q_x"]
    )

    def peak_one():
        r["tile2"][...] = peak_tile([jnp.max(r["top_h"][...]) * hid_s])
        start_y2()
        r["slots_y2"][0] = r["tile2"][...]

    def peak_two():
        finish_y2()
        r["mid2"][...] = jnp.max(r["slots_y2"][...], axis=0)
        start_x2()
        r["slots_x2"][0] = r["mid2"][...]

    def peak_three():
        loop(0, nc, hidden_out.arrive)
        finish_x2()
        top2 = jnp.max(r["slots_x2"][...], axis=0)
        r["mid3"][...] = top2
        hidden_inv = tile_scalar(1.0 / (top2 + tiny), 0) * hid_s

        def hidden_step(c):
            turned = dot(hidden_out.rows(c, 0), r["tab_h"][...])
            r["hid"][c] = soft(turned * hidden_inv)

        loop(0, nc, hidden_step)

    y_order = sorted(range(1, y_outer), key=lambda k: abs(2 * k - y_outer)) + [0]
    bufs = [r["out_part"], r["in_part"]]
    ones, twos, threes = r["y_one"], r["y_two"], r["y_three"]

    def y_near(i, k, o):
        j, to = lax.rem(y_hi + k, y_outer), lax.rem(y_lo + o, lanes)
        return remote(
            bufs[i].at[lanes * j + to], ones.at[i, k, o - 1], r["y_s1"].at[i],
            r["y_r1"].at[i, k], {"gy": lanes * y_hi + to},
        )

    def y_far(i, k):
        j = lax.rem(y_hi + k, y_outer)
        return remote(
            twos.at[i, k - 1], threes.at[i, k - 1], r["y_s2"].at[i],
            r["y_r2"].at[i], {"gy": lanes * j + y_lo},
        )

    def y_send(i):
        for k in y_order:
            for o in range(1, lanes):
                y_near(i, k, o).start()

    def y_sum(i, k):
        total = bufs[i][lanes * lax.rem(y_hi + k, y_outer) + y_lo].astype(F32)
        for o in range(1, lanes):
            total = total + ones[i, k, o - 1].astype(F32)
        return total

    def y_pass(i, k):
        take(ones.at[i, k], r["y_r1"].at[i, k])
        twos[i, k - 1] = y_sum(i, k).astype(BF16)
        y_far(i, k).start()

    def y_close(i):
        take(ones.at[i, 0], r["y_r1"].at[i, 0])
        total = y_sum(i, 0)
        take(threes.at[i], r["y_r2"].at[i])
        for k in y_order[:-1]:
            total = total + threes[i, k - 1].astype(F32)
        return total

    def out_step(b):
        cols = ds(b, band)
        total = jnp.zeros((total_t, band), F32)
        for c in range(nc):
            total = total + dot(r["hid"][c], wd[c, :, cols])
        r["out_part"][:, :, cols] = total.astype(BF16).reshape(ny, tl, band)

    def out_all():
        loop(0, nb, out_step)
        y_send(0)

    def out_pass():
        for k in y_order[:-1]:
            y_pass(0, k)

    def y_drain(i):
        take(ones.at[i], r["y_s1"].at[i])
        take(threes.at[i], r["y_s2"].at[i])

    def in_sum(c, rows):
        gate_sum = dot_t(grad_out.rows(c, 0), wg[c, rows, :]) * gate_unit
        return gate_sum + dot_t(grad_out.rows(c, 1), wu[c, rows, :]) * up_unit

    def in_step(c):
        grad_out.arrive(c)
        for b in range(nb):
            rows = slice(b * band, (b + 1) * band)
            r["acc"][:, rows] += in_sum(c, rows)

    def in_last():
        grad_out.arrive(nc - 1)
        for b in range(nb):
            rows = slice(b * band, (b + 1) * band)
            total = r["acc"][:, rows] + in_sum(nc - 1, rows)
            r["in_part"][:, :, rows] = total.astype(BF16).reshape(ny, tl, band)
        y_send(1)

    r["acc"][...] = jnp.zeros((total_t, wide), F32)

    def turn_tokens():
        for b in range(nb):
            cols = slice(b * band, (b + 1) * band)
            turned = dot(r["tok"][:, cols], r["tab_w"][...]) * tok_s
            r["tok_t"][cols, :] = turned.T.astype(BF16)

    def pipe(i):
        def both(lag, one, two):
            when((i >= lag) & (i < nc + lag), one, i - lag)
            when((i >= nc + lag) & (i < 2 * nc + lag), two, i - nc - lag)

        both(0, pre.turn, back.turn)
        if inside:
            when((i >= lead) & (i < lead + inside), g_forward, 1, i - lead + 1)
        when(i == nc - 1, cot_ready)
        both(-1, mm_pre, mm_back)
        both(LAG, act_hidden, act_grad)
        when(i == nc - 1 + LAG, peak_one)
        both(2 * LAG, hidden_out.forward, grad_out.forward)
        both(-2, cast_gate_up, cast_down)
        when(i == nc + 1 + LAG, peak_two)
        first_in = nc + 2 * LAG + 1
        when((i >= first_in) & (i < first_in + nc - 1), in_step, i - first_in)
        when(i == nc + 2 * LAG + 1, peak_three)
        when(i == nc + 2 * LAG + 2, out_all)
        when(i == nc + 2 * LAG + 3, turn_tokens)
        when(i == nc + 2 * LAG + 4, out_pass)

    cast_gate_up(0)
    mm_pre(0)
    (cast_gate_up(1) if nc > 1 else cast_down(0))
    loop(0, max(2 * nc + 2 * LAG, nc + 2 * LAG + 5), pipe)
    in_last()

    top2 = r["mid3"][...]
    hidden_unit = tile_scalar(top2 / fp_top, 0)
    out_scale = tile_scalar(top2[0:1, :] * top[3:4, :] / (fp_top * fp_top), 0)

    def gate_up_grads(c):
        for b in range(nb):
            rows = slice(b * band, (b + 1) * band)
            for i, weight in enumerate((wg, wu)):
                weight[c, rows, :] = (
                    dot(r["tok_t"][rows, :], grad_out.rows(c, i)) * tok_unit
                ).astype(BF16)

    def down_grads(c):
        turned = (dot(r["hid"][c], r["tab_h"][...]) * hid_s).T.astype(BF16)
        cot = all_cot[...].reshape(total_t, wide)
        wd[c] = (dot(turned, cot) * hidden_unit).astype(BF16)

    loop(0, nc, gate_up_grads)
    cuts = [nc * k // y_outer for k in range(y_outer + 1)]
    for n, k in enumerate(y_order):
        if k:
            y_pass(1, k)
        loop(cuts[n], cuts[n + 1], down_grads)
    r["output"][...] = (y_close(0) * out_scale).astype(BF16)
    pre.drain()
    back.drain()
    hidden_out.drain()
    grad_out.drain()
    for i in range(2):
        g_drain(i)
        y_drain(i)
    total = y_close(1)
    for b in range(nb):
        cols = slice(b * band, (b + 1) * band)
        r["input_grad"][:, cols] = (
            dot_wide(total[:, cols], r["tab_w"][...]) * tok_s
        ).astype(BF16)


def store_kernel(nc, piece, *refs):
    small, grads, outs, sems = refs[:2], refs[2:5], refs[5:10], refs[10]
    copies = [
        pltpu.make_async_copy(small[i], outs[i], sems.at[i, 0]) for i in range(2)
    ]
    for c in range(nc):
        cols = pl.ds(c * piece, piece)
        for i in range(3):
            dst = outs[2 + i].at[cols, :] if i == 2 else outs[2 + i].at[:, cols]
            copies.append(pltpu.make_async_copy(grads[i].at[c], dst, sems.at[2 + i, c]))
    for copy in copies:
        copy.start()
    for copy in copies:
        copy.wait()


def shards(nx, ny, tokens, cotangent, gate_weight, up_weight, down_weight):
    lanes = 1 << max((ny.bit_length() - 2) // 2, 0)
    tl, wide = tokens.shape
    hid = gate_weight.shape[1]
    piece = 256 if hid % 256 == 0 else hid
    band = 256 if wide % 256 == 0 else wide
    nc = hid // piece
    total_t = tl * ny
    tc = total_t // nx
    x_outer, y_outer = nx // CORES, ny // lanes
    dims = (nx, ny, lanes, tl, wide, hid, piece, band)
    ins = ["tokens", "cot", "gate", "up", "down"]
    outs = ["output", "input_grad", "wg", "wu", "wd"]
    tile = pltpu.VMEM((8, 128), F32)
    scratch = {
        "load": DMA((3, nc)), "own": DMA((2,)),
        "all_tok": pltpu.VMEM((ny, tl, wide), BF16),
        "all_cot": pltpu.VMEM((ny, tl, wide), BF16),
        "g_sf": DMA((2,)), "g_rf": DMA((2, y_outer - 1)),
        "g_sn": DMA((2,)), "g_rn": DMA((2,)),
        "tab_w": pltpu.VMEM((band, band), BF16),
        "tab_h": pltpu.VMEM((piece, piece), BF16),
        "tile": tile, "mid": tile, "tile2": tile, "mid2": tile, "mid3": tile,
        "slots_x": pltpu.VMEM((nx, 8, 128), F32),
        "slots_y": pltpu.VMEM((ny, 8, 128), F32),
        "slots_x2": pltpu.VMEM((nx, 8, 128), F32),
        "slots_y2": pltpu.VMEM((ny, 8, 128), F32),
        "p_x": DMA((2,)), "p_y": DMA((2,)), "q_x": DMA((2,)), "q_y": DMA((2,)),
        "tok": pltpu.VMEM((total_t, wide), BF16),
        "tok_t": pltpu.VMEM((wide, total_t), BF16),
        "slope": pltpu.VMEM((nc, 2, tc, piece), F32),
        "hid": pltpu.VMEM((nc, total_t, piece), BF16),
        "acc": pltpu.VMEM((total_t, wide), F32),
        "top_h": pltpu.VMEM((8, piece), F32),
        "out_part": pltpu.VMEM((ny, tl, wide), BF16),
        "in_part": pltpu.VMEM((ny, tl, wide), BF16),
        "y_one": pltpu.VMEM((2, y_outer, lanes - 1, tl, wide), BF16),
        "y_two": pltpu.VMEM((2, y_outer - 1, tl, wide), BF16),
        "y_three": pltpu.VMEM((2, y_outer - 1, tl, wide), BF16),
        "y_s1": DMA((2,)), "y_r1": DMA((2, y_outer)),
        "y_s2": DMA((2,)), "y_r2": DMA((2,)),
    }
    for tag, count in (("pre", 2), ("back", 1)):
        block = (count, tc, piece)
        scratch[tag + "_part"] = pltpu.VMEM((nc, nx) + block, F32)
        scratch[tag + "_first"] = pltpu.VMEM((nc, x_outer, CORES - 1) + block, F32)
        scratch[tag + "_second"] = pltpu.VMEM((nc, x_outer - 1) + block, BF16)
        scratch[tag + "_third"] = pltpu.VMEM((nc, x_outer - 1) + block, BF16)
        scratch[tag + "_s"] = DMA((2,))
        scratch[tag + "_r1"] = DMA((nc, x_outer))
        scratch[tag + "_r2"] = DMA((nc, x_outer - 1))
    for tag, count in (("act_h", 1), ("act_g", 2)):
        scratch[tag] = pltpu.VMEM((nc, nx, count, tc, piece), BF16)
        scratch[tag + "_s"] = DMA((2,))
        scratch[tag + "_rf"] = DMA((nc, x_outer - 1))
        scratch[tag + "_rn"] = DMA((nc,))
    names = tuple(ins + outs + list(scratch))
    small = jax.ShapeDtypeStruct(tokens.shape, BF16)
    small_vmem = pltpu.VMEM(tokens.shape, BF16)
    columns = pltpu.VMEM((nc, wide, piece), BF16)
    rows = pltpu.VMEM((nc, piece, wide), BF16)
    results = pl.pallas_call(
        functools.partial(layer_kernel, dims, names),
        out_shape=[small_vmem, small_vmem, columns, columns, rows],
        in_specs=[HBM] * 5,
        out_specs=[VMEM] * 5,
        scratch_shapes=list(scratch.values()),
        compiler_params=pltpu.CompilerParams(
            collective_id=0, has_side_effects=True, vmem_limit_bytes=VMEM_MIB * 2 ** 20
        ),
    )(tokens, cotangent, gate_weight, up_weight, down_weight)
    return pl.pallas_call(
        functools.partial(store_kernel, nc, piece),
        out_shape=[small, small] + [
            jax.ShapeDtypeStruct(w.shape, BF16)
            for w in (gate_weight, up_weight, down_weight)
        ],
        in_specs=[VMEM] * 5,
        out_specs=[HBM] * 5,
        scratch_shapes=[DMA((5, nc))],
        compiler_params=pltpu.CompilerParams(vmem_limit_bytes=STORE_MIB * 2 ** 20),
    )(*results)


def solution(mesh):
    in_specs = (P("gy", "gx"), P("gy", "gx"), P("gx", "gy"), P("gx", "gy"), P("gy", "gx"))
    out_specs = (P("gy", "gx"), P("gy", "gx"), P("gx", "gy"), P("gx", "gy"), P("gy", "gx"))
    nx, ny = mesh.shape["gx"], mesh.shape["gy"]
    return jax.shard_map(
        functools.partial(shards, nx, ny),
        mesh=mesh, in_specs=in_specs, out_specs=out_specs, check_vma=False,
    )
```

```python
import functools

import jax
import jax.numpy as jnp
from jax import lax
from jax.experimental import pallas as pl
from jax.experimental.pallas import tpu as pltpu
from jax.sharding import PartitionSpec as P

ROT_BLOCK = 128
HID_BLOCK = 64
CORES = 2
VMEM_MIB = 50
STORE_MIB = 12
LAG = 2
SPLIT = 1

fp_top = 448.0
tiny = 1e-06

MESH = pl.DeviceIdType.MESH
VMEM = pl.BlockSpec(memory_space=pltpu.VMEM)
HBM = pl.BlockSpec(memory_space=pltpu.HBM)
DMA = pltpu.SemaphoreType.DMA
F32 = jnp.float32
BF16 = jnp.bfloat16


def rot_table(size, block):
    shift = block.bit_length() - 1
    row = lax.broadcasted_iota(jnp.int32, (size, size), 0)
    col = lax.broadcasted_iota(jnp.int32, (size, size), 1)
    bits = row & col & (block - 1)
    bits = bits ^ (bits >> 4)
    bits = bits ^ (bits >> 2)
    bits = bits ^ (bits >> 1)
    sign = 1 - 2 * (bits & 1)
    return jnp.where((row >> shift) == (col >> shift), sign, 0).astype(F32).astype(BF16)


def dot(left, right):
    return jnp.dot(left, right, preferred_element_type=F32)


def dot_t(left, right):
    return lax.dot_general(
        left, right, (((1,), (1,)), ((), ())), preferred_element_type=F32
    )


def dot_wide(values, table):
    high = values.astype(BF16)
    rest = values - high.astype(F32)
    mid = rest.astype(BF16)
    low = (rest - mid.astype(F32)).astype(BF16)
    return dot(high, table) + (dot(mid, table) + dot(low, table))


def remote(src, dst, send, recv, target):
    return pltpu.make_async_remote_copy(
        src_ref=src, dst_ref=dst, send_sem=send, recv_sem=recv,
        device_id=target, device_id_type=MESH,
    )


def loop(low, high, body):
    def step(i, carry):
        body(i)
        return carry
    lax.fori_loop(low, high, step, 0)


def greet(nx, ny, gx, gy):
    barrier = pltpu.get_barrier_semaphore()
    for n, me, axis in ((nx, gx, "gx"), (ny, gy, "gy")):

        def hello(k, n=n, me=me, axis=axis):
            pl.semaphore_signal(
                barrier, inc=1, device_id={axis: lax.rem(me + k, n)}, device_id_type=MESH
            )

        loop(1, n, hello)
    return lambda: pl.semaphore_wait(barrier, nx - 1 + ny - 1)


def take(ref, sem):
    pltpu.make_async_copy(ref, ref, sem).wait()


def share_peaks(n, me, axis, slots, sems):
    def start(k):
        target = {axis: lax.rem(me + k, n)}
        remote(slots.at[0], slots.at[k], sems.at[0], sems.at[1], target).start()

    def finish():
        rest = slots.at[pl.ds(1, n - 1)]
        take(rest, sems.at[0])
        take(rest, sems.at[1])
        return jnp.max(slots[...], axis=0)

    return (lambda: loop(1, n, start)), finish


def fold(values):
    rows, cols = values.shape
    return jnp.max(jnp.abs(values).reshape(rows // 8, 8, cols), axis=0)


def ds(i, size):
    return pl.ds(pl.multiple_of(i * size, size), size)


def lane_ids():
    return lax.broadcasted_iota(jnp.int32, (1, 128), 1)


def peak_row(values):
    row = jnp.zeros((1, 128), F32)
    for i, value in enumerate(values):
        row = jnp.where(lane_ids() == i, value, row)
    return row


def lane_scalar(row, i):
    return jnp.max(jnp.where(lane_ids() == i, row, 0.0))


def layer_kernel(dims, names, *refs):
    nx, ny, lanes, tl, wide, hid, piece, band = dims
    r = dict(zip(names, refs))
    total_t = tl * ny
    hl, th = tl // 2, total_t // nx // 2
    nc = hid // piece
    nb = wide // band
    tail = min(SPLIT, nc)
    gx, gy = lax.axis_index("gx"), lax.axis_index("gy")
    tok_s, hid_s = ROT_BLOCK ** (-0.5), HID_BLOCK ** (-0.5)
    wg, wu, wd = r["wg"], r["wu"], r["wd"]
    all_tok, all_cot = r["all_tok"], r["all_cot"]

    def own_load(i, h):
        src, dst = ((r["tokens"], all_tok), (r["cot"], all_cot))[i]
        src = src.at[pl.ds(h * hl, hl)]
        return pltpu.make_async_copy(src, dst.at[h, gy], r["own"].at[i, h])

    own_load(0, 0).start()
    own_load(0, 1).start()
    greeted = greet(nx, ny, gx, gy)
    own_load(1, 0).start()
    own_load(1, 1).start()

    def load(i, c):
        cols = ds(c, piece)
        src, dst = [
            (r["gate"].at[:, cols], wg.at[c]),
            (r["up"].at[:, cols], wu.at[c]),
            (r["down"].at[cols, :], wd.at[c]),
        ][i]
        return pltpu.make_async_copy(src, dst, r["load"].at[i, c])

    def start_loads(c):
        for i in range(3):
            load(i, c).start()

    loop(0, nc, start_loads)
    r["tab_w"][...] = rot_table(band, ROT_BLOCK)
    r["tab_h"][...] = rot_table(piece, HID_BLOCK)
    own_load(0, 0).wait()
    own_load(0, 1).wait()
    tok_top = jnp.zeros((8, band), F32)
    for b in range(nb):
        cols = slice(b * band, (b + 1) * band)
        tok_top = jnp.maximum(tok_top, fold(dot(all_tok[:, gy, :, cols].reshape(tl, band), r["tab_w"][...])))

    def peak_step(c, tops):
        gate_top, up_top, down_top = tops
        for i in range(3):
            load(i, c).wait()
        for b in range(nb):
            rows = slice(b * band, (b + 1) * band)
            gate_top = jnp.maximum(gate_top, fold(dot(r["tab_w"][...], wg[c, rows, :])))
            up_top = jnp.maximum(up_top, fold(dot(r["tab_w"][...], wu[c, rows, :])))
            down_top = jnp.maximum(down_top, fold(dot(r["tab_h"][...], wd[c, :, rows])))
        return gate_top, up_top, down_top

    tops = (
        jnp.zeros((8, piece), F32), jnp.zeros((8, piece), F32), jnp.zeros((8, band), F32)
    )
    early = nc // 2
    tops = lax.fori_loop(0, early, peak_step, tops)
    greeted()

    y_outer = ny // lanes
    y_hi, y_lo = gy // lanes, lax.rem(gy, lanes)
    g_all = [all_tok, all_cot]

    relay = wide // 4
    cuts = pl.ds(0, wide - relay), pl.ds(wide - relay, relay)

    def g_far(i, p, k, slot):
        j = lax.rem(y_hi + k, y_outer)
        ref = g_all[i].at[:, slot, :, cuts[p]]
        recv = r["g_rf"].at[i, 0 if p else k]
        return remote(ref, ref, r["g_sf"].at[i, p], recv, {"gy": lanes * j + y_lo})

    def g_near(i, o, ref, recv):
        target = {"gy": lanes * y_hi + lax.rem(y_lo + o, lanes)}
        return remote(ref, ref, recv[0], recv[1], target)

    y_mid = sorted(range(1, y_outer), key=lambda k: abs(2 * k - y_outer))
    flip = 2 * y_hi // y_outer
    side = y_hi + flip * (y_outer - 1 - 2 * y_hi)

    def far_first(n):
        back = y_outer - 2 - y_hi + flip + (2 * flip - 1) * n
        return lax.rem(back + 2 * (y_outer - 1), y_outer - 1) + 1

    def near_first(n):
        paired = n < 2 * side
        step = jnp.where(paired, n // 2 + 1, n - side + 1)
        down = jnp.where(paired, 1 - 2 * (n % 2), -1) * (1 - 2 * flip)
        return lax.rem(down * step + y_outer, y_outer)

    def g_start(i):
        for o in range(1, lanes):
            g_near(i, o, g_all[i].at[:, gy], (r["g_sn"].at[i, 0], r["g_rn"].at[i, 0])).start()
        for n in range(y_outer - 1):
            g_far(i, 0, far_first(n), gy).start()

    def g_relay(i):
        for n in range(y_outer - 1):
            g_far(i, 1, far_first(n), gy).start()
        take(g_all[i].at[:, pl.ds(0, lanes - 1)], r["g_rn"].at[i, 0])
        for o in range(1, lanes):
            beside = lanes * y_hi + lax.rem(y_lo + o, lanes)
            for n in range(y_outer - 1):
                g_far(i, 1, far_first(n), beside).start()

    def g_forward(i, k):
        mine = lanes * lax.rem(y_hi + y_outer - k, y_outer) + y_lo
        g_far(i, 0, k, mine).wait_recv()
        ref = g_all[i].at[:, mine, :, cuts[0]]
        for o in range(1, lanes):
            g_near(i, o, ref, (r["g_sn"].at[i, 1], r["g_rn"].at[i, 1])).start()

    def g_blocks(i, p, count):
        return g_all[i].at[:, pl.ds(0, count), :, cuts[p]]

    def g_finish(i):
        take(g_blocks(i, 0, (y_outer - 1) * (lanes - 1)), r["g_rn"].at[i, 1])
        take(g_blocks(i, 1, (y_outer - 1) * lanes), r["g_rf"].at[i, 0])

    def g_drain(i):
        take(g_all[i].at[:, pl.ds(0, lanes - 1)], r["g_sn"].at[i, 0])
        take(g_blocks(i, 0, (y_outer - 1) * (lanes - 1)), r["g_sn"].at[i, 1])
        take(g_blocks(i, 0, y_outer - 1), r["g_sf"].at[i, 0])
        take(g_blocks(i, 1, (y_outer - 1) * lanes), r["g_sf"].at[i, 1])

    g_start(0)

    tops = lax.fori_loop(early, nc, peak_step, tops)
    start_x, finish_x = share_peaks(nx, gx, "gx", r["slots_x"], r["p_x"])
    start_y, finish_y = share_peaks(ny, gy, "gy", r["slots_y"], r["p_y"])
    r["slots_x"][0] = peak_row([
        jnp.max(tok_top) * tok_s, jnp.max(tops[0]) * tok_s,
        jnp.max(tops[1]) * tok_s, jnp.max(tops[2]) * hid_s,
    ])
    start_x()
    g_relay(0)
    g_forward(0, near_first(0))
    r["slots_y"][0] = finish_x()
    start_y()
    for n in range(1, y_outer - 1):
        g_forward(0, near_first(n))
    top = finish_y()
    own_load(1, 0).wait()
    own_load(1, 1).wait()
    g_start(1)
    inverse = 1.0 / (top + tiny)
    unit = top / fp_top
    pair = lane_scalar(top, 0) * top / (fp_top * fp_top)
    tok_inv = lane_scalar(inverse, 0) * tok_s
    gate_inv = lane_scalar(inverse, 1) * tok_s
    up_inv = lane_scalar(inverse, 2) * tok_s
    down_inv = lane_scalar(inverse, 3) * hid_s
    tok_unit, gate_unit, up_unit, down_unit = (lane_scalar(unit, i) for i in range(4))
    gate_scale, up_scale = lane_scalar(pair, 1), lane_scalar(pair, 2)

    def soft(values):
        return (fp_top * jnp.tanh(values)).astype(BF16)

    def cast_gate_up(c):
        for b in range(nb):
            rows = slice(b * band, (b + 1) * band)
            wg[c, rows, :] = soft(dot(r["tab_w"][...], wg[c, rows, :]) * gate_inv)
            wu[c, rows, :] = soft(dot(r["tab_w"][...], wu[c, rows, :]) * up_inv)

    def cast_down(c):
        for b in range(nb):
            rows = slice(b * band, (b + 1) * band)
            wd[c, :, rows] = soft(dot(r["tab_h"][...], wd[c, :, rows]) * down_inv)

    x_outer = nx // CORES
    x_hi, x_lo = gx // CORES, lax.rem(gx, CORES)
    x_order = list(range(1, x_outer)) + [0]

    def span(h):
        return pl.ds(0, 2) if h is None else pl.ds(h, 1)

    def order(c, h):
        return c + tail if h == 1 else c

    class Sums:
        def __init__(self, tag, count):
            self.count = count
            self.part, self.first = r[tag + "_part"], r[tag + "_first"]
            self.second, self.third = r[tag + "_second"], r[tag + "_third"]
            self.s1, self.r1 = r[tag + "_s"].at[0], r[tag + "_r1"]
            self.s2, self.r2 = r[tag + "_s"].at[1], r[tag + "_r2"]

        def far(self, c, h, k):
            j = lax.rem(x_hi + k, x_outer)
            return remote(
                self.second.at[c, k - 1, span(h)], self.third.at[c, k - 1, span(h)],
                self.s2, self.r2.at[order(c, h), k - 1], {"gx": CORES * j + x_lo},
            )

        def send(self, c, h):
            for k in x_order:
                j = lax.rem(x_hi + k, x_outer)
                for o in range(1, CORES):
                    to = lax.rem(x_lo + o, CORES)
                    remote(
                        self.part.at[c, span(h), CORES * j + to],
                        self.first.at[c, k, o - 1, span(h)],
                        self.s1, self.r1.at[order(c, h)], {"gx": CORES * x_hi + to},
                    ).start()

        def near_sum(self, c, h, k, i):
            slot = CORES * lax.rem(x_hi + k, x_outer) + x_lo
            total = self.part[c, span(h), slot, i]
            for o in range(1, CORES):
                total = total + self.first[c, k, o - 1, span(h), i]
            return total

        def turn(self, c, h):
            whole = self.first.at[c, pl.ds(0, x_outer), pl.ds(0, CORES - 1), span(h)]
            take(whole, self.r1.at[order(c, h)])
            for k in x_order[:-1]:
                for i in range(self.count):
                    self.second[c, k - 1, span(h), i] = self.near_sum(c, h, k, i).astype(
                        BF16
                    )
                self.far(c, h, k).start()

        def close(self, c, h):
            for k in x_order[:-1]:
                self.far(c, h, k).wait_recv()

        def drain(self):
            take(self.first, self.s1)
            take(self.third, self.s2)

        def full(self, c, h, i):
            total = self.near_sum(c, h, 0, i)
            for k in x_order[:-1]:
                total = total + self.third[c, k - 1, span(h), i].astype(F32)
            return total.reshape(-1, piece)

    class Spread:
        def __init__(self, tag):
            self.act = r[tag]
            self.sf, self.rf = r[tag + "_s"].at[0], r[tag + "_rf"]
            self.sn, self.rn = r[tag + "_s"].at[1], r[tag + "_rn"]

        def far(self, c, h, k, slot):
            ref = self.act.at[c, span(h), slot]
            target = {"gx": CORES * lax.rem(x_hi + k, x_outer) + x_lo}
            return remote(ref, ref, self.sf, self.rf.at[order(c, h), k - 1], target)

        def near(self, c, h, o, slot):
            ref = self.act.at[c, span(h), slot]
            target = {"gx": CORES * x_hi + lax.rem(x_lo + o, CORES)}
            return remote(ref, ref, self.sn, self.rn.at[order(c, h)], target)

        def put(self, c, h, i, values):
            self.act[c, span(h), gx, i] = values.astype(BF16).reshape(-1, th, piece)

        def send(self, c, h):
            for k in range(1, x_outer):
                self.far(c, h, k, gx).start()
            for o in range(1, CORES):
                self.near(c, h, o, gx).start()

        def forward(self, c, h):
            for k in range(1, x_outer):
                mine = CORES * lax.rem(x_hi + x_outer - k, x_outer) + x_lo
                self.far(c, h, k, mine).wait_recv()
                for o in range(1, CORES):
                    self.near(c, h, o, mine).start()

        def arrive(self, c, h=None):
            some = pl.ds(0, x_outer * (CORES - 1))
            take(self.act.at[c, span(h), some], self.rn.at[order(c, h)])

        def drain(self):
            take(self.act.at[:, :, pl.ds(0, x_outer - 1)], self.sf)
            take(self.act.at[:, :, pl.ds(0, x_outer * (CORES - 1))], self.sn)

        def rows(self, c, i, h=None):
            return self.act[c, span(h), :, i].reshape(-1, piece)

    pre, back = Sums("pre", 2), Sums("back", 1)
    hidden_out, grad_out = Spread("act_h"), Spread("act_g")

    def mm_pre(c, h):
        for i, weight in enumerate((wg, wu)):
            total = dot(r["tok"][...], weight[c])
            pre.part[c, :, :, i] = total.reshape(2, nx, th, piece)
        pre.send(c, h)

    def mm_back(c, h):
        cot = all_cot[span(h)].reshape(-1, wide)
        back.part[c, span(h), :, 0] = dot_t(cot, wd[c]).reshape(-1, nx, th, piece)
        back.send(c, h)

    def act_hidden(c, h):
        pre.close(c, h)
        gate_pre = pre.full(c, h, 0) * gate_scale
        up_pre = pre.full(c, h, 1) * up_scale
        sig = jax.nn.sigmoid(gate_pre)
        hidden = (gate_pre * sig * up_pre).astype(BF16)
        hidden_out.put(c, h, 0, hidden)
        hidden_out.send(c, h)
        slope = up_pre * sig * (1.0 + gate_pre * (1.0 - sig))
        r["slope"][c, 0] = slope.reshape(2, th, piece)
        r["slope"][c, 1] = (gate_pre * sig).reshape(2, th, piece)
        r["top_h"][...] = jnp.maximum(
            r["top_h"][...], fold(dot(hidden, r["tab_h"][...]))
        )

    def act_grad(c, h):
        back.close(c, h)
        grad = dot_wide(back.full(c, h, 0) * down_unit, r["tab_h"][...]) * hid_s
        for i in range(2):
            slope = r["slope"][c, i, span(h)].reshape(-1, piece)
            grad_out.put(c, h, i, grad * slope)
        grad_out.send(c, h)

    r["top_h"][...] = jnp.zeros((8, piece), F32)

    def when(cond, body, *args):
        @pl.when(cond)
        def _():
            body(*args)

    lead = 3
    inside = max(0, min(y_outer - 1, nc - lead))

    def forward_cot(n):
        when(n == 0, g_relay, 1)
        g_forward(1, near_first(n))

    def cot_ready():
        if not inside:
            g_relay(1)
        for n in range(inside, y_outer - 1):
            g_forward(1, near_first(n))
        g_finish(1)

    start_y2, finish_y2 = share_peaks(ny, gy, "gy", r["slots_y2"], r["q_y"])
    start_x2, finish_x2 = share_peaks(nx, gx, "gx", r["slots_x2"], r["q_x"])

    def peak_one():
        r["slots_y2"][0] = peak_row([jnp.max(r["top_h"][...]) * hid_s])
        start_y2()

    def peak_two():
        r["slots_x2"][0] = finish_y2()
        start_x2()

    def peak_three():
        loop(0, nc, hidden_out.arrive)
        top2 = finish_x2()
        r["mid"][...] = top2
        hidden_inv = lane_scalar(1.0 / (top2 + tiny), 0) * hid_s

        def hidden_step(c):
            turned = dot(hidden_out.rows(c, 0), r["tab_h"][...])
            r["hid"][c] = soft(turned * hidden_inv)

        loop(0, nc, hidden_step)

    y_order = y_mid + [0]
    def y_block(i, d):
        return r["in_part"].at[i - 1, d] if i else r["out_part"].at[:, d]

    def y_refs(name):
        return [r[name + "_o"]] + [r[name + "_i"].at[p] for p in range(2)]

    ones, twos, threes = (y_refs(name) for name in ("y_one", "y_two", "y_three"))

    def y_near(i, k, o):
        j, to = lax.rem(y_hi + k, y_outer), lax.rem(y_lo + o, lanes)
        return remote(
            y_block(i, lanes * j + to), ones[i].at[k, o - 1], r["y_s1"].at[i],
            r["y_r1"].at[i, k], {"gy": lanes * y_hi + to},
        )

    def y_far(i, k):
        j = lax.rem(y_hi + k, y_outer)
        return remote(
            twos[i].at[k - 1], threes[i].at[k - 1], r["y_s2"].at[i],
            r["y_r2"].at[i], {"gy": lanes * j + y_lo},
        )

    def y_send(i):
        for k in y_order:
            for o in range(1, lanes):
                y_near(i, k, o).start()

    def y_sum(i, k):
        total = y_block(i, lanes * lax.rem(y_hi + k, y_outer) + y_lo)[...].astype(F32)
        for o in range(1, lanes):
            total = total + ones[i][k, o - 1].astype(F32)
        return total

    def y_pass(i, k):
        take(ones[i].at[k], r["y_r1"].at[i, k])
        twos[i][k - 1] = y_sum(i, k).astype(BF16)
        y_far(i, k).start()

    def y_close(i):
        take(ones[i].at[0], r["y_r1"].at[i, 0])
        total = y_sum(i, 0)
        take(threes[i], r["y_r2"].at[i])
        for k in y_order[:-1]:
            total = total + threes[i][k - 1].astype(F32)
        return total

    def out_step(b):
        cols = ds(b, band)
        total = jnp.zeros((total_t, band), F32)
        for c in range(nc):
            total = total + dot(r["hid"][c], wd[c, :, cols])
        r["out_part"][:, :, :, cols] = total.astype(BF16).reshape(2, ny, hl, band)

    def out_all():
        loop(0, nb, out_step)
        y_send(0)

    def y_drain(i):
        take(ones[i], r["y_s1"].at[i])
        take(threes[i], r["y_s2"].at[i])

    def in_sum(c, h, rows):
        gate_sum = dot_t(grad_out.rows(c, 0, h), wg[c, rows, :]) * gate_unit
        total = gate_sum + dot_t(grad_out.rows(c, 1, h), wu[c, rows, :]) * up_unit
        return total.reshape(-1, total_t // 2, band)

    def in_step(c, h):
        grad_out.arrive(c, h)
        for b in range(nb):
            rows = slice(b * band, (b + 1) * band)
            r["acc"][span(h), :, rows] += in_sum(c, h, rows)

    def in_last(h):
        grad_out.arrive(nc - 1, h)
        for b in range(nb):
            rows = slice(b * band, (b + 1) * band)
            total = r["acc"][span(h), :, rows] + in_sum(nc - 1, h, rows)
            r["in_part"][h, :, :, rows] = total.astype(BF16).reshape(ny, hl, band)
        y_send(1 + h)

    r["acc"][...] = jnp.zeros((2, total_t // 2, wide), F32)

    def down_grads(low, high):
        hidden_unit = lane_scalar(r["mid"][...] / fp_top, 0)

        def one(c):
            turned = (dot(r["hid"][c], r["tab_h"][...]) * hid_s).T.astype(BF16)
            cot = all_cot[...].reshape(total_t, wide)
            wd[c] = (dot(turned, cot) * hidden_unit).astype(BF16)

        loop(low, high, one)

    def turn_tokens():
        for b in range(nb):
            cols = slice(b * band, (b + 1) * band)
            turned = dot(r["tok"][:, cols], r["tab_w"][...]) * tok_s
            r["tok_t"][cols, :] = turned.T.astype(BF16)

    head = nc - tail
    parts = [(0, head, None), (head, tail, 0), (head + tail, tail, 1)]

    def pipe(i):
        def back_items(first, body):
            for low, count, h in parts:
                if count:
                    at = first + low
                    c = i - at + (0 if h is None else head)
                    when((i >= at) & (i < at + count), body, c, h)

        def both(lag, one, two):
            when((i >= lag) & (i < nc + lag), one, i - lag, None)
            back_items(nc + lag, two)

        both(0, pre.turn, back.turn)
        if inside:
            when((i >= lead) & (i < lead + inside), forward_cot, i - lead)
        when(i == nc - 1, cot_ready)
        both(-1, mm_pre, mm_back)
        both(LAG, act_hidden, act_grad)
        when(i == nc - 1 + LAG, peak_one)
        both(2 * LAG, hidden_out.forward, grad_out.forward)
        when(i + 2 < nc, cast_gate_up, i + 2)
        when((i + 2 >= nc) & (i + 2 < 2 * nc), cast_down, i + 2 - nc)
        when(i == nc + 1 + LAG, peak_two)
        for low, count, h in parts:
            at = first_in + low
            c = i - at + (0 if h is None else head)
            steps = count if h is None else count - 1
            if steps:
                when((i >= at) & (i < at + steps), in_step, c, h)
        when(i == first_in + nc - 1, in_last, 0)
        when(i == first_in, peak_three)
        when(i == first_in + 1, out_all)
        when(i == min(lead, nc - 1), turn_tokens)
        for n, k in enumerate(y_mid):
            when(i == first_in + 4 + n, y_pass, 0, k)

    first_in = nc + 2 * LAG + 1
    cast_gate_up(0)
    g_finish(0)
    for b in range(nb):
        cols = slice(b * band, (b + 1) * band)
        raw = all_tok[:, :, :, cols].reshape(total_t, band)
        r["tok"][:, cols] = soft(dot(raw, r["tab_w"][...]) * tok_inv)
    mm_pre(0, None)
    (cast_gate_up(1) if nc > 1 else cast_down(0))
    loop(0, max(first_in + nc + tail - 1, first_in + 4 + len(y_mid)), pipe)
    in_last(1)

    top2 = r["mid"][...]
    out_scale = lane_scalar(top2 * lane_scalar(top, 3) / (fp_top * fp_top), 0)

    def run_jobs(some):
        for body in (down_grads, gate_up_grads):
            at = [c for b, c in some if b is body]
            if at:
                body(at[0], at[-1] + 1)

    def gate_up_chunk(c):
        for b in range(nb):
            rows = slice(b * band, (b + 1) * band)
            for i, weight in enumerate((wg, wu)):
                weight[c, rows, :] = (
                    dot(r["tok_t"][rows, :], grad_out.rows(c, i)) * tok_unit
                ).astype(BF16)

    def gate_up_grads(low, high):
        loop(low, high, gate_up_chunk)

    passes = [(1 + h, k) for h in range(2) for k in y_mid]
    jobs = [(down_grads, c) for c in range(nc)] + [(gate_up_grads, c) for c in range(nc)]
    ahead, after = len(jobs) * 2 // 7, len(jobs) // 5
    between = len(jobs) - ahead - after
    done = 0
    for n, (i, k) in enumerate(passes):
        due = ahead + between * n // (len(passes) - 1)
        run_jobs(jobs[done:due])
        done = due
        y_pass(i, k)
    run_jobs(jobs[done:])
    r["output"][...] = (y_close(0).reshape(tl, wide) * out_scale).astype(BF16)
    pre.drain()
    back.drain()
    hidden_out.drain()
    grad_out.drain()
    for i in range(2):
        g_drain(i)
    for i in range(3):
        y_drain(i)
    for p in range(2):
        total = y_close(1 + p)
        for b in range(nb):
            cols = slice(b * band, (b + 1) * band)
            turned = dot_wide(total[:, cols], r["tab_w"][...]) * tok_s
            r["input_grad"][pl.ds(p * hl, hl), cols] = turned.astype(BF16)


def store_kernel(nc, piece, *refs):
    small, grads, outs, sems = refs[:2], refs[2:5], refs[5:10], refs[10]
    copies = [
        pltpu.make_async_copy(small[i], outs[i], sems.at[i, 0]) for i in range(2)
    ]
    for c in range(nc):
        cols = pl.ds(c * piece, piece)
        for i in range(3):
            dst = outs[2 + i].at[cols, :] if i == 2 else outs[2 + i].at[:, cols]
            copies.append(pltpu.make_async_copy(grads[i].at[c], dst, sems.at[2 + i, c]))
    for copy in copies:
        copy.start()
    for copy in copies:
        copy.wait()


def shards(nx, ny, tokens, cotangent, gate_weight, up_weight, down_weight):
    lanes = 1 << max((ny.bit_length() - 2) // 2, 0)
    tl, wide = tokens.shape
    hid = gate_weight.shape[1]
    piece = 256 if hid % 256 == 0 else hid
    band = 256 if wide % 256 == 0 else wide
    nc = hid // piece
    total_t = tl * ny
    hl, th = tl // 2, total_t // nx // 2
    tail = min(SPLIT, nc)
    x_outer, y_outer = nx // CORES, ny // lanes
    dims = (nx, ny, lanes, tl, wide, hid, piece, band)
    ins = ["tokens", "cot", "gate", "up", "down"]
    outs = ["output", "input_grad", "wg", "wu", "wd"]
    scratch = {
        "load": DMA((3, nc)), "own": DMA((2, 2)),
        "all_tok": pltpu.VMEM((2, ny, hl, wide), BF16),
        "all_cot": pltpu.VMEM((2, ny, hl, wide), BF16),
        "g_sf": DMA((2, 2)), "g_rf": DMA((2, y_outer)),
        "g_sn": DMA((2, 2)), "g_rn": DMA((2, 2)),
        "tab_w": pltpu.VMEM((band, band), BF16),
        "tab_h": pltpu.VMEM((piece, piece), BF16),
        "mid": pltpu.VMEM((1, 128), F32),
        "slots_x": pltpu.VMEM((nx, 1, 128), F32),
        "slots_y": pltpu.VMEM((ny, 1, 128), F32),
        "slots_x2": pltpu.VMEM((nx, 1, 128), F32),
        "slots_y2": pltpu.VMEM((ny, 1, 128), F32),
        "p_x": DMA((2,)), "p_y": DMA((2,)), "q_x": DMA((2,)), "q_y": DMA((2,)),
        "tok": pltpu.VMEM((total_t, wide), BF16),
        "tok_t": pltpu.VMEM((wide, total_t), BF16),
        "slope": pltpu.VMEM((nc, 2, 2, th, piece), F32),
        "hid": pltpu.VMEM((nc, total_t, piece), BF16),
        "acc": pltpu.VMEM((2, total_t // 2, wide), F32),
        "top_h": pltpu.VMEM((8, piece), F32),
        "out_part": pltpu.VMEM((2, ny, hl, wide), BF16),
        "in_part": pltpu.VMEM((2, ny, hl, wide), BF16),
        "y_one_o": pltpu.VMEM((y_outer, lanes - 1, 2, hl, wide), BF16),
        "y_two_o": pltpu.VMEM((y_outer - 1, 2, hl, wide), BF16),
        "y_three_o": pltpu.VMEM((y_outer - 1, 2, hl, wide), BF16),
        "y_one_i": pltpu.VMEM((2, y_outer, lanes - 1, hl, wide), BF16),
        "y_two_i": pltpu.VMEM((2, y_outer - 1, hl, wide), BF16),
        "y_three_i": pltpu.VMEM((2, y_outer - 1, hl, wide), BF16),
        "y_s1": DMA((3,)), "y_r1": DMA((3, y_outer)),
        "y_s2": DMA((3,)), "y_r2": DMA((3,)),
    }
    for tag, count, items in (("pre", 2, nc), ("back", 1, nc + tail)):
        block = (2, count, th, piece)
        scratch[tag + "_part"] = pltpu.VMEM((nc, 2, nx, count, th, piece), F32)
        scratch[tag + "_first"] = pltpu.VMEM((nc, x_outer, CORES - 1) + block, F32)
        scratch[tag + "_second"] = pltpu.VMEM((nc, x_outer - 1) + block, BF16)
        scratch[tag + "_third"] = pltpu.VMEM((nc, x_outer - 1) + block, BF16)
        scratch[tag + "_s"] = DMA((2,))
        scratch[tag + "_r1"] = DMA((items,))
        scratch[tag + "_r2"] = DMA((items, x_outer - 1))
    for tag, count, items in (("act_h", 1, nc), ("act_g", 2, nc + tail)):
        scratch[tag] = pltpu.VMEM((nc, 2, nx, count, th, piece), BF16)
        scratch[tag + "_s"] = DMA((2,))
        scratch[tag + "_rf"] = DMA((items, x_outer - 1))
        scratch[tag + "_rn"] = DMA((items,))
    names = tuple(ins + outs + list(scratch))
    small = jax.ShapeDtypeStruct(tokens.shape, BF16)
    small_vmem = pltpu.VMEM(tokens.shape, BF16)
    columns = pltpu.VMEM((nc, wide, piece), BF16)
    rows = pltpu.VMEM((nc, piece, wide), BF16)
    results = pl.pallas_call(
        functools.partial(layer_kernel, dims, names),
        out_shape=[small_vmem, small_vmem, columns, columns, rows],
        in_specs=[HBM] * 5,
        out_specs=[VMEM] * 5,
        scratch_shapes=list(scratch.values()),
        compiler_params=pltpu.CompilerParams(
            collective_id=0, has_side_effects=True, vmem_limit_bytes=VMEM_MIB * 2 ** 20
        ),
    )(tokens, cotangent, gate_weight, up_weight, down_weight)
    return pl.pallas_call(
        functools.partial(store_kernel, nc, piece),
        out_shape=[small, small] + [
            jax.ShapeDtypeStruct(w.shape, BF16)
            for w in (gate_weight, up_weight, down_weight)
        ],
        in_specs=[VMEM] * 5,
        out_specs=[HBM] * 5,
        scratch_shapes=[DMA((5, nc))],
        compiler_params=pltpu.CompilerParams(vmem_limit_bytes=STORE_MIB * 2 ** 20),
    )(*results)


def solution(mesh):
    in_specs = (P("gy", "gx"), P("gy", "gx"), P("gx", "gy"), P("gx", "gy"), P("gy", "gx"))
    out_specs = (P("gy", "gx"), P("gy", "gx"), P("gx", "gy"), P("gx", "gy"), P("gy", "gx"))
    nx, ny = mesh.shape["gx"], mesh.shape["gy"]
    return jax.shard_map(
        functools.partial(shards, nx, ny),
        mesh=mesh, in_specs=in_specs, out_specs=out_specs, check_vma=False,
    )
```

```python
import functools

import jax
import jax.numpy as jnp
from jax import lax
from jax.experimental import pallas as pl
from jax.experimental.pallas import tpu as pltpu
from jax.sharding import PartitionSpec as P

ROT_BLOCK = 128
HID_BLOCK = 64
CORES = 2
VMEM_MIB = 50
STORE_MIB = 12
LAG = 2
SPLIT = 1

fp_top = 448.0
tiny = 1e-06

MESH = pl.DeviceIdType.MESH
VMEM = pl.BlockSpec(memory_space=pltpu.VMEM)
HBM = pl.BlockSpec(memory_space=pltpu.HBM)
DMA = pltpu.SemaphoreType.DMA
F32 = jnp.float32
BF16 = jnp.bfloat16


def rot_table(size, block):
    shift = block.bit_length() - 1
    row = lax.broadcasted_iota(jnp.int32, (size, size), 0)
    col = lax.broadcasted_iota(jnp.int32, (size, size), 1)
    bits = row & col & (block - 1)
    bits = bits ^ (bits >> 4)
    bits = bits ^ (bits >> 2)
    bits = bits ^ (bits >> 1)
    sign = 1 - 2 * (bits & 1)
    return jnp.where((row >> shift) == (col >> shift), sign, 0).astype(F32).astype(BF16)


def dot(left, right):
    return jnp.dot(left, right, preferred_element_type=F32)


def dot_t(left, right):
    return lax.dot_general(
        left, right, (((1,), (1,)), ((), ())), preferred_element_type=F32
    )


def dot_wide(values, table):
    high = values.astype(BF16)
    rest = values - high.astype(F32)
    mid = rest.astype(BF16)
    low = (rest - mid.astype(F32)).astype(BF16)
    return dot(high, table) + (dot(mid, table) + dot(low, table))


def remote(src, dst, send, recv, target):
    return pltpu.make_async_remote_copy(
        src_ref=src, dst_ref=dst, send_sem=send, recv_sem=recv,
        device_id=target, device_id_type=MESH,
    )


def loop(low, high, body):
    def step(i, carry):
        body(i)
        return carry
    lax.fori_loop(low, high, step, 0)


def greet(nx, ny, gx, gy):
    barrier = pltpu.get_barrier_semaphore()
    for n, me, axis in ((nx, gx, "gx"), (ny, gy, "gy")):

        def hello(k, n=n, me=me, axis=axis):
            pl.semaphore_signal(
                barrier, inc=1, device_id={axis: lax.rem(me + k, n)}, device_id_type=MESH
            )

        loop(1, n, hello)
    return lambda: pl.semaphore_wait(barrier, nx - 1 + ny - 1)


def take(ref, sem):
    pltpu.make_async_copy(ref, ref, sem).wait()


def share_peaks(n, me, axis, slots, sems):
    def start(k):
        target = {axis: lax.rem(me + k, n)}
        remote(slots.at[0], slots.at[k], sems.at[0], sems.at[1], target).start()

    def finish():
        rest = slots.at[pl.ds(1, n - 1)]
        take(rest, sems.at[0])
        take(rest, sems.at[1])
        return jnp.max(slots[...], axis=0)

    return (lambda: loop(1, n, start)), finish


def fold(values):
    rows, cols = values.shape
    return jnp.max(jnp.abs(values).reshape(rows // 8, 8, cols), axis=0)


def ds(i, size):
    return pl.ds(pl.multiple_of(i * size, size), size)


def lane_ids():
    return lax.broadcasted_iota(jnp.int32, (1, 128), 1)


def peak_row(values):
    row = jnp.zeros((1, 128), F32)
    for i, value in enumerate(values):
        row = jnp.where(lane_ids() == i, value, row)
    return row


def lane_scalar(row, i):
    return jnp.max(jnp.where(lane_ids() == i, row, 0.0))


def layer_kernel(dims, names, *refs):
    nx, ny, lanes, tl, wide, hid, piece, band = dims
    r = dict(zip(names, refs))
    total_t = tl * ny
    hl, th = tl // 2, total_t // nx // 2
    nc = hid // piece
    nb = wide // band
    tail = min(SPLIT, nc)
    gx, gy = lax.axis_index("gx"), lax.axis_index("gy")
    tok_s, hid_s = ROT_BLOCK ** (-0.5), HID_BLOCK ** (-0.5)
    wg, wu, wd = r["wg"], r["wu"], r["wd"]
    all_tok, all_cot = r["all_tok"], r["all_cot"]

    def own_load(i, h):
        src, dst = ((r["tokens"], all_tok), (r["cot"], all_cot))[i]
        src = src.at[pl.ds(h * hl, hl)]
        return pltpu.make_async_copy(src, dst.at[h, gy], r["own"].at[i, h])

    own_load(0, 0).start()
    own_load(0, 1).start()
    greeted = greet(nx, ny, gx, gy)
    own_load(1, 0).start()
    own_load(1, 1).start()

    def load(i, c):
        cols = ds(c, piece)
        src, dst = [
            (r["gate"].at[:, cols], wg.at[c]),
            (r["up"].at[:, cols], wu.at[c]),
            (r["down"].at[cols, :], wd.at[c]),
        ][i]
        return pltpu.make_async_copy(src, dst, r["load"].at[i, c])

    def start_loads(c):
        for i in range(3):
            load(i, c).start()

    loop(0, nc, start_loads)
    r["tab_w"][...] = rot_table(band, ROT_BLOCK)
    r["tab_h"][...] = rot_table(piece, HID_BLOCK)
    own_load(0, 0).wait()
    own_load(0, 1).wait()
    tok_top = jnp.zeros((8, band), F32)
    for b in range(nb):
        cols = slice(b * band, (b + 1) * band)
        tok_top = jnp.maximum(tok_top, fold(dot(all_tok[:, gy, :, cols].reshape(tl, band), r["tab_w"][...])))

    def peak_step(c, tops):
        gate_top, up_top, down_top = tops
        for i in range(3):
            load(i, c).wait()
        for b in range(nb):
            rows = slice(b * band, (b + 1) * band)
            gate_top = jnp.maximum(gate_top, fold(dot(r["tab_w"][...], wg[c, rows, :])))
            up_top = jnp.maximum(up_top, fold(dot(r["tab_w"][...], wu[c, rows, :])))
            down_top = jnp.maximum(down_top, fold(dot(r["tab_h"][...], wd[c, :, rows])))
        return gate_top, up_top, down_top

    tops = (
        jnp.zeros((8, piece), F32), jnp.zeros((8, piece), F32), jnp.zeros((8, band), F32)
    )
    early = nc // 2
    tops = lax.fori_loop(0, early, peak_step, tops)
    greeted()

    y_outer = ny // lanes
    y_hi, y_lo = gy // lanes, lax.rem(gy, lanes)
    g_all = [all_tok, all_cot]

    relay = 3 * wide // 8 // 128 * 128
    cuts = pl.ds(0, wide - relay), pl.ds(wide - relay, relay)

    def g_far(i, p, k, slot):
        j = lax.rem(y_hi + k, y_outer)
        ref = g_all[i].at[:, slot, :, cuts[p]]
        recv = r["g_rf"].at[i, 0 if p else k]
        return remote(ref, ref, r["g_sf"].at[i, p], recv, {"gy": lanes * j + y_lo})

    def g_near(i, o, ref, recv):
        target = {"gy": lanes * y_hi + lax.rem(y_lo + o, lanes)}
        return remote(ref, ref, recv[0], recv[1], target)

    y_mid = sorted(range(1, y_outer), key=lambda k: abs(2 * k - y_outer))
    flip = 2 * y_hi // y_outer
    side = y_hi + flip * (y_outer - 1 - 2 * y_hi)

    def far_first(n):
        back = y_outer - 2 - y_hi + flip + (2 * flip - 1) * n
        return lax.rem(back + 2 * (y_outer - 1), y_outer - 1) + 1

    def near_first(n):
        paired = n < 2 * side
        step = jnp.where(paired, n // 2 + 1, n - side + 1)
        down = jnp.where(paired, 1 - 2 * (n % 2), -1) * (1 - 2 * flip)
        return lax.rem(down * step + y_outer, y_outer)

    def g_start(i):
        for o in range(1, lanes):
            g_near(i, o, g_all[i].at[:, gy], (r["g_sn"].at[i, 0], r["g_rn"].at[i, 0])).start()
        for n in range(y_outer - 1):
            g_far(i, 0, far_first(n), gy).start()

    def g_relay(i):
        for n in range(y_outer - 1):
            g_far(i, 1, far_first(n), gy).start()
        take(g_all[i].at[:, pl.ds(0, lanes - 1)], r["g_rn"].at[i, 0])
        for o in range(1, lanes):
            beside = lanes * y_hi + lax.rem(y_lo + o, lanes)
            for n in range(y_outer - 1):
                g_far(i, 1, far_first(n), beside).start()

    def g_forward(i, k):
        mine = lanes * lax.rem(y_hi + y_outer - k, y_outer) + y_lo
        g_far(i, 0, k, mine).wait_recv()
        ref = g_all[i].at[:, mine, :, cuts[0]]
        for o in range(1, lanes):
            g_near(i, o, ref, (r["g_sn"].at[i, 1], r["g_rn"].at[i, 1])).start()

    def g_blocks(i, p, count):
        return g_all[i].at[:, pl.ds(0, count), :, cuts[p]]

    def g_finish(i):
        take(g_blocks(i, 0, (y_outer - 1) * (lanes - 1)), r["g_rn"].at[i, 1])
        take(g_blocks(i, 1, (y_outer - 1) * lanes), r["g_rf"].at[i, 0])

    def g_drain(i):
        take(g_all[i].at[:, pl.ds(0, lanes - 1)], r["g_sn"].at[i, 0])
        take(g_blocks(i, 0, (y_outer - 1) * (lanes - 1)), r["g_sn"].at[i, 1])
        take(g_blocks(i, 0, y_outer - 1), r["g_sf"].at[i, 0])
        take(g_blocks(i, 1, (y_outer - 1) * lanes), r["g_sf"].at[i, 1])

    g_start(0)

    tops = lax.fori_loop(early, nc, peak_step, tops)
    start_x, finish_x = share_peaks(nx, gx, "gx", r["slots_x"], r["p_x"])
    start_y, finish_y = share_peaks(ny, gy, "gy", r["slots_y"], r["p_y"])
    r["slots_x"][0] = peak_row([
        jnp.max(tok_top) * tok_s, jnp.max(tops[0]) * tok_s,
        jnp.max(tops[1]) * tok_s, jnp.max(tops[2]) * hid_s,
    ])
    start_x()
    g_relay(0)
    g_forward(0, near_first(0))
    r["slots_y"][0] = finish_x()
    start_y()
    for n in range(1, y_outer - 1):
        g_forward(0, near_first(n))
    top = finish_y()
    own_load(1, 0).wait()
    own_load(1, 1).wait()
    g_start(1)
    inverse = 1.0 / (top + tiny)
    unit = top / fp_top
    pair = lane_scalar(top, 0) * top / (fp_top * fp_top)
    tok_inv = lane_scalar(inverse, 0) * tok_s
    gate_inv = lane_scalar(inverse, 1) * tok_s
    up_inv = lane_scalar(inverse, 2) * tok_s
    down_inv = lane_scalar(inverse, 3) * hid_s
    tok_unit, gate_unit, up_unit, down_unit = (lane_scalar(unit, i) for i in range(4))
    gate_scale, up_scale = lane_scalar(pair, 1), lane_scalar(pair, 2)

    def soft(values):
        return (fp_top * jnp.tanh(values)).astype(BF16)

    def cast_gate_up(c):
        for b in range(nb):
            rows = slice(b * band, (b + 1) * band)
            wg[c, rows, :] = soft(dot(r["tab_w"][...], wg[c, rows, :]) * gate_inv)
            wu[c, rows, :] = soft(dot(r["tab_w"][...], wu[c, rows, :]) * up_inv)

    def cast_down(c):
        for b in range(nb):
            rows = slice(b * band, (b + 1) * band)
            wd[c, :, rows] = soft(dot(r["tab_h"][...], wd[c, :, rows]) * down_inv)

    x_outer = nx // CORES
    x_hi, x_lo = gx // CORES, lax.rem(gx, CORES)
    x_order = list(range(1, x_outer)) + [0]

    def span(h):
        return pl.ds(0, 2) if h is None else pl.ds(h, 1)

    def order(c, h):
        return c + tail if h == 1 else c

    class Sums:
        def __init__(self, tag, count):
            self.count = count
            self.part, self.first = r[tag + "_part"], r[tag + "_first"]
            self.second, self.third = r[tag + "_second"], r[tag + "_third"]
            self.s1, self.r1 = r[tag + "_s"].at[0], r[tag + "_r1"]
            self.s2, self.r2 = r[tag + "_s"].at[1], r[tag + "_r2"]

        def far(self, c, h, k):
            j = lax.rem(x_hi + k, x_outer)
            return remote(
                self.second.at[c, k - 1, span(h)], self.third.at[c, k - 1, span(h)],
                self.s2, self.r2.at[order(c, h), k - 1], {"gx": CORES * j + x_lo},
            )

        def send(self, c, h):
            for k in x_order:
                j = lax.rem(x_hi + k, x_outer)
                for o in range(1, CORES):
                    to = lax.rem(x_lo + o, CORES)
                    remote(
                        self.part.at[c, span(h), CORES * j + to],
                        self.first.at[c, k, o - 1, span(h)],
                        self.s1, self.r1.at[order(c, h)], {"gx": CORES * x_hi + to},
                    ).start()

        def near_sum(self, c, h, k, i):
            slot = CORES * lax.rem(x_hi + k, x_outer) + x_lo
            total = self.part[c, span(h), slot, i]
            for o in range(1, CORES):
                total = total + self.first[c, k, o - 1, span(h), i]
            return total

        def turn(self, c, h):
            whole = self.first.at[c, pl.ds(0, x_outer), pl.ds(0, CORES - 1), span(h)]
            take(whole, self.r1.at[order(c, h)])
            for k in x_order[:-1]:
                for i in range(self.count):
                    self.second[c, k - 1, span(h), i] = self.near_sum(c, h, k, i).astype(
                        BF16
                    )
                self.far(c, h, k).start()

        def close(self, c, h):
            for k in x_order[:-1]:
                self.far(c, h, k).wait_recv()

        def drain(self):
            take(self.first, self.s1)
            take(self.third, self.s2)

        def full(self, c, h, i):
            total = self.near_sum(c, h, 0, i)
            for k in x_order[:-1]:
                total = total + self.third[c, k - 1, span(h), i].astype(F32)
            return total.reshape(-1, piece)

    class Spread:
        def __init__(self, tag):
            self.act = r[tag]
            self.sf, self.rf = r[tag + "_s"].at[0], r[tag + "_rf"]
            self.sn, self.rn = r[tag + "_s"].at[1], r[tag + "_rn"]

        def far(self, c, h, k, slot):
            ref = self.act.at[c, span(h), slot]
            target = {"gx": CORES * lax.rem(x_hi + k, x_outer) + x_lo}
            return remote(ref, ref, self.sf, self.rf.at[order(c, h), k - 1], target)

        def near(self, c, h, o, slot):
            ref = self.act.at[c, span(h), slot]
            target = {"gx": CORES * x_hi + lax.rem(x_lo + o, CORES)}
            return remote(ref, ref, self.sn, self.rn.at[order(c, h)], target)

        def put(self, c, h, i, values):
            self.act[c, span(h), gx, i] = values.astype(BF16).reshape(-1, th, piece)

        def send(self, c, h):
            for k in range(1, x_outer):
                self.far(c, h, k, gx).start()
            for o in range(1, CORES):
                self.near(c, h, o, gx).start()

        def forward(self, c, h):
            for k in range(1, x_outer):
                mine = CORES * lax.rem(x_hi + x_outer - k, x_outer) + x_lo
                self.far(c, h, k, mine).wait_recv()
                for o in range(1, CORES):
                    self.near(c, h, o, mine).start()

        def arrive(self, c, h=None):
            some = pl.ds(0, x_outer * (CORES - 1))
            take(self.act.at[c, span(h), some], self.rn.at[order(c, h)])

        def drain(self):
            take(self.act.at[:, :, pl.ds(0, x_outer - 1)], self.sf)
            take(self.act.at[:, :, pl.ds(0, x_outer * (CORES - 1))], self.sn)

        def rows(self, c, i, h=None):
            return self.act[c, span(h), :, i].reshape(-1, piece)

    pre, back = Sums("pre", 2), Sums("back", 1)
    hidden_out, grad_out = Spread("act_h"), Spread("act_g")

    def mm_pre(c, h):
        for i, weight in enumerate((wg, wu)):
            total = dot(r["tok"][...], weight[c])
            pre.part[c, :, :, i] = total.reshape(2, nx, th, piece)
        pre.send(c, h)

    def mm_back(c, h):
        cot = all_cot[span(h)].reshape(-1, wide)
        back.part[c, span(h), :, 0] = dot_t(cot, wd[c]).reshape(-1, nx, th, piece)
        back.send(c, h)

    def act_hidden(c, h):
        pre.close(c, h)
        gate_pre = pre.full(c, h, 0) * gate_scale
        up_pre = pre.full(c, h, 1) * up_scale
        sig = jax.nn.sigmoid(gate_pre)
        hidden = (gate_pre * sig * up_pre).astype(BF16)
        hidden_out.put(c, h, 0, hidden)
        hidden_out.send(c, h)
        slope = up_pre * sig * (1.0 + gate_pre * (1.0 - sig))
        r["slope"][c, 0] = slope.reshape(2, th, piece)
        r["slope"][c, 1] = (gate_pre * sig).reshape(2, th, piece)
        r["top_h"][...] = jnp.maximum(
            r["top_h"][...], fold(dot(hidden, r["tab_h"][...]))
        )

    def act_grad(c, h):
        back.close(c, h)
        grad = dot_wide(back.full(c, h, 0) * down_unit, r["tab_h"][...]) * hid_s
        for i in range(2):
            slope = r["slope"][c, i, span(h)].reshape(-1, piece)
            grad_out.put(c, h, i, grad * slope)
        grad_out.send(c, h)

    r["top_h"][...] = jnp.zeros((8, piece), F32)

    def when(cond, body, *args):
        @pl.when(cond)
        def _():
            body(*args)

    lead = 3
    inside = max(0, min(y_outer - 1, nc - lead))

    def forward_cot(n):
        when(n == 0, g_relay, 1)
        g_forward(1, near_first(n))

    def cot_ready():
        if not inside:
            g_relay(1)
        for n in range(inside, y_outer - 1):
            g_forward(1, near_first(n))
        g_finish(1)

    start_y2, finish_y2 = share_peaks(ny, gy, "gy", r["slots_y2"], r["q_y"])
    start_x2, finish_x2 = share_peaks(nx, gx, "gx", r["slots_x2"], r["q_x"])

    def peak_one():
        r["slots_y2"][0] = peak_row([jnp.max(r["top_h"][...]) * hid_s])
        start_y2()

    def peak_two():
        r["slots_x2"][0] = finish_y2()
        start_x2()

    def peak_three():
        loop(0, nc, hidden_out.arrive)
        top2 = finish_x2()
        r["mid"][...] = top2
        hidden_inv = lane_scalar(1.0 / (top2 + tiny), 0) * hid_s

        def hidden_step(c):
            turned = dot(hidden_out.rows(c, 0), r["tab_h"][...])
            r["hid"][c] = soft(turned * hidden_inv)

        loop(0, nc, hidden_step)

    y_order = y_mid + [0]
    def y_block(i, d):
        return r["in_part"].at[i - 1, d] if i else r["out_part"].at[:, d]

    def y_refs(name):
        return [r[name + "_o"]] + [r[name + "_i"].at[p] for p in range(2)]

    ones, twos, threes = (y_refs(name) for name in ("y_one", "y_two", "y_three"))

    def y_near(i, k, o):
        j, to = lax.rem(y_hi + k, y_outer), lax.rem(y_lo + o, lanes)
        return remote(
            y_block(i, lanes * j + to), ones[i].at[k, o - 1], r["y_s1"].at[i],
            r["y_r1"].at[i, k], {"gy": lanes * y_hi + to},
        )

    def y_far(i, k):
        j = lax.rem(y_hi + k, y_outer)
        return remote(
            twos[i].at[k - 1], threes[i].at[k - 1], r["y_s2"].at[i],
            r["y_r2"].at[i], {"gy": lanes * j + y_lo},
        )

    def y_send(i, order):
        for k in order:
            for o in range(1, lanes):
                y_near(i, k, o).start()

    def y_sum(i, k):
        total = y_block(i, lanes * lax.rem(y_hi + k, y_outer) + y_lo)[...].astype(F32)
        for o in range(1, lanes):
            total = total + ones[i][k, o - 1].astype(F32)
        return total

    def y_pass(i, k):
        take(ones[i].at[k], r["y_r1"].at[i, k])
        twos[i][k - 1] = y_sum(i, k).astype(BF16)
        y_far(i, k).start()

    def y_close(i):
        take(ones[i].at[0], r["y_r1"].at[i, 0])
        total = y_sum(i, 0)
        take(threes[i], r["y_r2"].at[i])
        for k in y_order[:-1]:
            total = total + threes[i][k - 1].astype(F32)
        return total

    def out_step(b):
        cols = ds(b, band)
        total = jnp.zeros((total_t, band), F32)
        for c in range(nc):
            total = total + dot(r["hid"][c], wd[c, :, cols])
        r["out_part"][:, :, :, cols] = total.astype(BF16).reshape(2, ny, hl, band)

    def out_all():
        loop(0, nb, out_step)
        y_send(0, y_order)

    def y_drain(i):
        take(ones[i], r["y_s1"].at[i])
        take(threes[i], r["y_s2"].at[i])

    def in_sum(c, h, rows):
        gate_sum = dot_t(grad_out.rows(c, 0, h), wg[c, rows, :]) * gate_unit
        total = gate_sum + dot_t(grad_out.rows(c, 1, h), wu[c, rows, :]) * up_unit
        return total.reshape(-1, total_t // 2, band)

    def in_step(c, h):
        grad_out.arrive(c, h)
        for b in range(nb):
            rows = slice(b * band, (b + 1) * band)
            r["acc"][span(h), :, rows] += in_sum(c, h, rows)

    def in_last(h):
        grad_out.arrive(nc - 1, h)
        for b in range(nb):
            rows = slice(b * band, (b + 1) * band)
            total = r["acc"][span(h), :, rows] + in_sum(nc - 1, h, rows)
            r["in_part"][h, :, :, rows] = total.astype(BF16).reshape(ny, hl, band)
        y_send(1 + h, y_mid)

    r["acc"][...] = jnp.zeros((2, total_t // 2, wide), F32)

    def down_grads(low, high):
        hidden_unit = lane_scalar(r["mid"][...] / fp_top, 0)

        def one(c):
            turned = (dot(r["hid"][c], r["tab_h"][...]) * hid_s).T.astype(BF16)
            cot = all_cot[...].reshape(total_t, wide)
            wd[c] = (dot(turned, cot) * hidden_unit).astype(BF16)

        loop(low, high, one)

    def turn_tokens():
        for b in range(nb):
            cols = slice(b * band, (b + 1) * band)
            turned = dot(r["tok"][:, cols], r["tab_w"][...]) * tok_s
            r["tok_t"][cols, :] = turned.T.astype(BF16)

    head = nc - tail
    parts = [(0, head, None), (head, tail, 0), (head + tail, tail, 1)]

    def pipe(i):
        def back_items(first, body):
            for low, count, h in parts:
                if count:
                    at = first + low
                    c = i - at + (0 if h is None else head)
                    when((i >= at) & (i < at + count), body, c, h)

        def both(lag, one, two):
            when((i >= lag) & (i < nc + lag), one, i - lag, None)
            back_items(nc + lag, two)

        both(0, pre.turn, back.turn)
        if inside:
            when((i >= lead) & (i < lead + inside), forward_cot, i - lead)
        when(i == nc - 1, cot_ready)
        both(-1, mm_pre, mm_back)
        both(LAG, act_hidden, act_grad)
        when(i == nc - 1 + LAG, peak_one)
        both(2 * LAG, hidden_out.forward, grad_out.forward)
        when(i + 2 < nc, cast_gate_up, i + 2)
        when((i + 2 >= nc) & (i + 2 < 2 * nc), cast_down, i + 2 - nc)
        when(i == nc + 1 + LAG, peak_two)
        for low, count, h in parts:
            at = first_in + low
            c = i - at + (0 if h is None else head)
            steps = count if h is None else count - 1
            if steps:
                when((i >= at) & (i < at + steps), in_step, c, h)
        when(i == first_in + nc - 1, in_last, 0)
        when(i == first_in, peak_three)
        when(i == first_in + 1, out_all)
        when(i == min(lead, nc - 1), turn_tokens)
        for n, k in enumerate(y_mid):
            when(i == first_in + 4 + n, y_pass, 0, k)

    first_in = nc + 2 * LAG + 1
    cast_gate_up(0)
    g_finish(0)
    for b in range(nb):
        cols = slice(b * band, (b + 1) * band)
        raw = all_tok[:, :, :, cols].reshape(total_t, band)
        r["tok"][:, cols] = soft(dot(raw, r["tab_w"][...]) * tok_inv)
    mm_pre(0, None)
    (cast_gate_up(1) if nc > 1 else cast_down(0))
    loop(0, max(first_in + nc + tail - 1, first_in + 4 + len(y_mid)), pipe)
    in_last(1)
    y_send(1, [0])
    y_send(2, [0])

    top2 = r["mid"][...]
    out_scale = lane_scalar(top2 * lane_scalar(top, 3) / (fp_top * fp_top), 0)

    def run_jobs(some):
        for body in (down_grads, gate_up_grads):
            at = [c for b, c in some if b is body]
            if at:
                body(at[0], at[-1] + 1)

    def gate_up_chunk(c):
        for b in range(nb):
            rows = slice(b * band, (b + 1) * band)
            for i, weight in enumerate((wg, wu)):
                weight[c, rows, :] = (
                    dot(r["tok_t"][rows, :], grad_out.rows(c, i)) * tok_unit
                ).astype(BF16)

    def gate_up_grads(low, high):
        loop(low, high, gate_up_chunk)

    passes = [(1 + h, k) for h in range(2) for k in y_mid]
    jobs = [(down_grads, c) for c in range(nc)] + [(gate_up_grads, c) for c in range(nc)]
    ahead, after = len(jobs) * 3 // 14, len(jobs) * 2 // 7
    between = len(jobs) - ahead - after
    done = 0
    for n, (i, k) in enumerate(passes):
        due = ahead + between * n // (len(passes) - 1)
        run_jobs(jobs[done:due])
        done = due
        y_pass(i, k)
    run_jobs(jobs[done:])
    r["output"][...] = (y_close(0).reshape(tl, wide) * out_scale).astype(BF16)
    pre.drain()
    back.drain()
    hidden_out.drain()
    grad_out.drain()
    for i in range(2):
        g_drain(i)
    for i in range(3):
        y_drain(i)
    for p in range(2):
        total = y_close(1 + p)
        for b in range(nb):
            cols = slice(b * band, (b + 1) * band)
            turned = dot_wide(total[:, cols], r["tab_w"][...]) * tok_s
            r["input_grad"][pl.ds(p * hl, hl), cols] = turned.astype(BF16)


def store_kernel(nc, piece, *refs):
    small, grads, outs, sems = refs[:2], refs[2:5], refs[5:10], refs[10]
    copies = [
        pltpu.make_async_copy(small[i], outs[i], sems.at[i, 0]) for i in range(2)
    ]
    for c in range(nc):
        cols = pl.ds(c * piece, piece)
        for i in range(3):
            dst = outs[2 + i].at[cols, :] if i == 2 else outs[2 + i].at[:, cols]
            copies.append(pltpu.make_async_copy(grads[i].at[c], dst, sems.at[2 + i, c]))
    for copy in copies:
        copy.start()
    for copy in copies:
        copy.wait()


def shards(nx, ny, tokens, cotangent, gate_weight, up_weight, down_weight):
    lanes = 1 << max((ny.bit_length() - 2) // 2, 0)
    tl, wide = tokens.shape
    hid = gate_weight.shape[1]
    piece = 256 if hid % 256 == 0 else hid
    band = 256 if wide % 256 == 0 else wide
    nc = hid // piece
    total_t = tl * ny
    hl, th = tl // 2, total_t // nx // 2
    tail = min(SPLIT, nc)
    x_outer, y_outer = nx // CORES, ny // lanes
    dims = (nx, ny, lanes, tl, wide, hid, piece, band)
    ins = ["tokens", "cot", "gate", "up", "down"]
    outs = ["output", "input_grad", "wg", "wu", "wd"]
    scratch = {
        "load": DMA((3, nc)), "own": DMA((2, 2)),
        "all_tok": pltpu.VMEM((2, ny, hl, wide), BF16),
        "all_cot": pltpu.VMEM((2, ny, hl, wide), BF16),
        "g_sf": DMA((2, 2)), "g_rf": DMA((2, y_outer)),
        "g_sn": DMA((2, 2)), "g_rn": DMA((2, 2)),
        "tab_w": pltpu.VMEM((band, band), BF16),
        "tab_h": pltpu.VMEM((piece, piece), BF16),
        "mid": pltpu.VMEM((1, 128), F32),
        "slots_x": pltpu.VMEM((nx, 1, 128), F32),
        "slots_y": pltpu.VMEM((ny, 1, 128), F32),
        "slots_x2": pltpu.VMEM((nx, 1, 128), F32),
        "slots_y2": pltpu.VMEM((ny, 1, 128), F32),
        "p_x": DMA((2,)), "p_y": DMA((2,)), "q_x": DMA((2,)), "q_y": DMA((2,)),
        "tok": pltpu.VMEM((total_t, wide), BF16),
        "tok_t": pltpu.VMEM((wide, total_t), BF16),
        "slope": pltpu.VMEM((nc, 2, 2, th, piece), F32),
        "hid": pltpu.VMEM((nc, total_t, piece), BF16),
        "acc": pltpu.VMEM((2, total_t // 2, wide), F32),
        "top_h": pltpu.VMEM((8, piece), F32),
        "out_part": pltpu.VMEM((2, ny, hl, wide), BF16),
        "in_part": pltpu.VMEM((2, ny, hl, wide), BF16),
        "y_one_o": pltpu.VMEM((y_outer, lanes - 1, 2, hl, wide), BF16),
        "y_two_o": pltpu.VMEM((y_outer - 1, 2, hl, wide), BF16),
        "y_three_o": pltpu.VMEM((y_outer - 1, 2, hl, wide), BF16),
        "y_one_i": pltpu.VMEM((2, y_outer, lanes - 1, hl, wide), BF16),
        "y_two_i": pltpu.VMEM((2, y_outer - 1, hl, wide), BF16),
        "y_three_i": pltpu.VMEM((2, y_outer - 1, hl, wide), BF16),
        "y_s1": DMA((3,)), "y_r1": DMA((3, y_outer)),
        "y_s2": DMA((3,)), "y_r2": DMA((3,)),
    }
    for tag, count, items in (("pre", 2, nc), ("back", 1, nc + tail)):
        block = (2, count, th, piece)
        scratch[tag + "_part"] = pltpu.VMEM((nc, 2, nx, count, th, piece), F32)
        scratch[tag + "_first"] = pltpu.VMEM((nc, x_outer, CORES - 1) + block, F32)
        scratch[tag + "_second"] = pltpu.VMEM((nc, x_outer - 1) + block, BF16)
        scratch[tag + "_third"] = pltpu.VMEM((nc, x_outer - 1) + block, BF16)
        scratch[tag + "_s"] = DMA((2,))
        scratch[tag + "_r1"] = DMA((items,))
        scratch[tag + "_r2"] = DMA((items, x_outer - 1))
    for tag, count, items in (("act_h", 1, nc), ("act_g", 2, nc + tail)):
        scratch[tag] = pltpu.VMEM((nc, 2, nx, count, th, piece), BF16)
        scratch[tag + "_s"] = DMA((2,))
        scratch[tag + "_rf"] = DMA((items, x_outer - 1))
        scratch[tag + "_rn"] = DMA((items,))
    names = tuple(ins + outs + list(scratch))
    small = jax.ShapeDtypeStruct(tokens.shape, BF16)
    small_vmem = pltpu.VMEM(tokens.shape, BF16)
    columns = pltpu.VMEM((nc, wide, piece), BF16)
    rows = pltpu.VMEM((nc, piece, wide), BF16)
    results = pl.pallas_call(
        functools.partial(layer_kernel, dims, names),
        out_shape=[small_vmem, small_vmem, columns, columns, rows],
        in_specs=[HBM] * 5,
        out_specs=[VMEM] * 5,
        scratch_shapes=list(scratch.values()),
        compiler_params=pltpu.CompilerParams(
            collective_id=0, has_side_effects=True, vmem_limit_bytes=VMEM_MIB * 2 ** 20
        ),
    )(tokens, cotangent, gate_weight, up_weight, down_weight)
    return pl.pallas_call(
        functools.partial(store_kernel, nc, piece),
        out_shape=[small, small] + [
            jax.ShapeDtypeStruct(w.shape, BF16)
            for w in (gate_weight, up_weight, down_weight)
        ],
        in_specs=[VMEM] * 5,
        out_specs=[HBM] * 5,
        scratch_shapes=[DMA((5, nc))],
        compiler_params=pltpu.CompilerParams(vmem_limit_bytes=STORE_MIB * 2 ** 20),
    )(*results)


def solution(mesh):
    in_specs = (P("gy", "gx"), P("gy", "gx"), P("gx", "gy"), P("gx", "gy"), P("gy", "gx"))
    out_specs = (P("gy", "gx"), P("gy", "gx"), P("gx", "gy"), P("gx", "gy"), P("gy", "gx"))
    nx, ny = mesh.shape["gx"], mesh.shape["gy"]
    return jax.shard_map(
        functools.partial(shards, nx, ny),
        mesh=mesh, in_specs=in_specs, out_specs=out_specs, check_vma=False,
    )
```
